32 devices in a mesh: row: 8 (over y, x, core), col: 4 (over z).
Axes of the slice: x: 2, y: 2, z: 4, core: 2. Of those that a mesh axis runs over, the one named last changes fastest.
Arguments:
- tile_u: float32 [8, 16, 2048, 128], P('row', 'col'), may hold values from -6 to 6
- tile_v: float32 [8, 16, 2048, 128], P('row', 'col'), may hold values from -1.5 to 1.5
- row_panel_u: float32 [8, 2048, 128], P('row', 'col'), may hold values from -6 to 6
- row_panel_v: float32 [8, 2048, 128], P('row', 'col'), may hold values from -0.125 to 0.125
- col_panel_u: float32 [16, 2048, 128], P('row', 'col'), may hold values from -6 to 6
- col_panel_v: float32 [16, 2048, 128], P('row', 'col'), may hold values from -0.125 to 0.125
- diag_inverse: float32 [2048, 2048], P('col'), may hold values from -0.15 to 2, as said below
- sketch: float32 [2048, 128], replicated, may hold values from -0.125 to 0.125
Outputs:
- new_u: float32 [8, 16, 2048, 128], P('row', 'col')
- new_v: float32 [8, 16, 2048, 128], P('row', 'col')
The draws below stay inside these ranges and needn't reach their ends.
Inputs may be any that keep to these rules, and one draw needn't show every extreme that they name: `diag_inverse`: lower triangular; the diagonal lies between 0.5 and 2, the entries below it between -0.15 and 0.15.
All inputs are finite; a program needn't handle non-finite values.
Results may differ from the reference program's by a relative error of at most 0.0003.
Values sent between devices are 32-bit elements; how exact they have to be, the bound alone decides.
No kernel may reach another device: no remote copies, remote signals or barrier semaphores. Data moves between devices by JAX's collectives and lax.ppermute only.
A program may use at most 128 MiB of HBM per device.

```python
import math
import jax
import jax.numpy as jnp
from jax import lax

B = 2048
K = 128
RT = 8
CT = 16


def draw_diag_inverse(key, part):
    first_key, second_key = jax.random.split(jax.random.fold_in(key, 17))
    diagonal = jax.random.uniform(first_key, (B,), jnp.float32, 0.5, 2.0)
    strict = jax.random.normal(second_key, (B, B), jnp.float32) / math.sqrt(B)
    strict = jnp.clip(strict, -0.15, 0.15)
    return jnp.tril(strict, -1) + jnp.diag(diagonal)


def block_scale(own_key, extent, pieces, low, largest):
    level, own = 1.0, jax.random.fold_in(own_key, 6)
    for axis_at, parts in pieces:
        steps = jnp.exp(jax.random.uniform(jax.random.fold_in(own, axis_at), (parts,), jnp.float32, low / len(pieces), largest / len(pieces)))
        level = level * jnp.repeat(steps, extent[axis_at] // parts).reshape([-1 if axis == axis_at else 1 for axis in range(len(extent))])
    return level


def scatter_about(stream_key, dims, deviation, bound, shards=(), dtype=jnp.bfloat16):
    result = jax.random.normal(stream_key, dims, jnp.float32) * deviation
    if len(shards) > 0:
        result = block_scale(stream_key, dims, shards, -0.22, 0.18) * result
    return jnp.clip(result, min=-bound, max=bound).astype(dtype)


def setup_inputs(seed: int = 0) -> dict:
    splits = jax.random.split(jax.random.key(seed), 9)
    return {
        "tile_u": scatter_about(splits[0], (RT, CT, B, K), 1.0, 6.0, ((0, 8), (1, 4)), jnp.float32),
        "tile_v": scatter_about(splits[1], (RT, CT, B, K), 0.25, 1.5, ((0, 8), (1, 4)), jnp.float32),
        "row_panel_u": scatter_about(splits[2], (RT, B, K), 1.0, 6.0, ((0, 8), (1, 4)), jnp.float32),
        "row_panel_v": scatter_about(splits[3], (RT, B, K), B ** -0.5, 0.125, ((0, 8), (1, 4)), jnp.float32),
        "col_panel_u": scatter_about(splits[4], (CT, B, K), 1.0, 6.0, ((0, 8), (1, 4)), jnp.float32),
        "col_panel_v": scatter_about(splits[5], (CT, B, K), B ** -0.5, 0.125, ((0, 8), (1, 4)), jnp.float32),
        "diag_inverse": draw_diag_inverse(jax.random.fold_in(splits[8], 71), 0),
        "sketch": scatter_about(splits[7], (B, K), B ** -0.5, 0.125, (), jnp.float32),
    }


highest = lax.Precision.HIGHEST

def recompress(tile_u, tile_v, row_u, cores, col_u, sketch):
    branch = -jnp.einsum('iak,ijkl->ijal', row_u, cores, precision=highest)
    left_side = jnp.concatenate([tile_u, branch], axis=-1)
    right_side = jnp.concatenate([tile_v, jnp.broadcast_to(col_u[None], tile_v.shape)], axis=-1)
    projected = jnp.einsum('ijar,ak->ijrk', right_side, sketch, precision=highest)
    sample = jnp.einsum('ijar,ijrk->ijak', left_side, projected, precision=highest)
    gram_matrix = jnp.einsum('ijak,ijal->ijkl', sample, sample, precision=highest)
    factor = jnp.linalg.cholesky(gram_matrix)
    solved_t = jax.scipy.linalg.solve_triangular(factor, jnp.swapaxes(sample, -1, -2), lower=True)
    basis = jnp.swapaxes(solved_t, -1, -2)
    coefficients = jnp.einsum('ijar,ijak->ijrk', left_side, basis, precision=highest)
    scaling = math.sqrt(tile_u.shape[2])
    new_v = jnp.einsum('ijar,ijrk->ijak', right_side, coefficients, precision=highest) / scaling
    return (basis * scaling, new_v)

def reference(tile_u, tile_v, row_panel_u, row_panel_v, col_panel_u, col_panel_v, diag_inverse, sketch):
    row_solved = jnp.einsum('ab,tbk->tak', diag_inverse, row_panel_v, precision=highest)
    col_solved = jnp.einsum('ab,tbk->tak', diag_inverse, col_panel_v, precision=highest)

    def one_row(entries):
        row_tiles_u, row_tiles_v, panel_u, panel_v = entries
        cores = jnp.einsum('ak,jal->jkl', panel_v, col_solved, precision=highest)
        result_u, result_v = recompress(row_tiles_u[None], row_tiles_v[None], panel_u[None], cores[None], col_panel_u, sketch)
        return (result_u[0], result_v[0])
    new_u, new_v = lax.map(one_row, (tile_u, tile_v, row_panel_u, row_solved))
    return (new_u, new_v)
```

```python
import functools
import math

import jax
import jax.numpy as jnp
from jax import lax
from jax.experimental import pallas as pl
from jax.experimental.pallas import tpu as pltpu
from jax.sharding import PartitionSpec as P

f32, bf16 = jnp.float32, jnp.bfloat16
ANY, VMEM = pl.ANY, pltpu.VMEM
NT = (((1,), (1,)), ((), ()))
NN = (((1,), (0,)), ((), ()))
TN = (((0,), (0,)), ((), ()))


def mm(a, b, dims):
    return lax.dot_general(a, b, dims, preferred_element_type=f32)


def halves(x):
    hi = x.astype(bf16)
    return hi, (x - hi.astype(f32)).astype(bf16)


def beside(x):
    return jnp.concatenate(halves(x), axis=1)


def doubled_rows(x):
    both = beside(x)
    return jnp.concatenate([both, both], axis=0)


def doubled_columns(x):
    hi, lo = halves(x)
    return jnp.concatenate([jnp.concatenate([hi, hi], axis=1), jnp.concatenate([lo, lo], axis=1)], axis=0)


def fold(x):
    w = x.shape[1] // 2
    return x[:, :w] + x[:, w:]


def product(a, b):
    return fold(mm(beside(a), doubled_rows(b), NN))


def product_nt(a, b):
    return fold(mm(beside(a), doubled_columns(b), NT))


def product_tn(a, b):
    x = fold(mm(beside(a), beside(b), TN))
    h = x.shape[0] // 2
    return x[:h] + x[h:]


def thirds(x):
    a = x.astype(bf16).astype(f32)
    r = x - a
    b = r.astype(bf16).astype(f32)
    return a, b, r - b


def eliminate(work, tiles, k):
    b = 8
    row = lax.broadcasted_iota(jnp.int32, (b, k), 0)
    for top in range(0, k, b):
        left, right, cols, scale = [], [], [], []
        for t in range(tiles):
            x = work[t, top : top + b, :]
            left.append(x[:, :k])
            right.append(x[:, k:])
            cols.append([jnp.broadcast_to(x[:, top + j : top + j + 1], (b, k)) for j in range(b)])
            scale.append(jnp.zeros((b, k), f32))
        for j in range(b):
            for t in range(tiles):
                pivot = jnp.broadcast_to(cols[t][j][j : j + 1, :], (b, k))
                inverse = 1.0 / pivot
                scale[t] = jnp.where(row == j, inverse, scale[t])
                if j + 1 < b:
                    m = jnp.where(row > j, cols[t][j] * inverse, 0.0)
                    for u in range(j + 1, b):
                        cols[t][u] = cols[t][u] - m * cols[t][u][j : j + 1, :]
                    left[t] = left[t] - m * left[t][j : j + 1, :]
                    right[t] = right[t] - m * right[t][j : j + 1, :]
        for t in range(tiles):
            work[t, top : top + b, k:] = right[t] * jnp.sqrt(scale[t])
        if top + b < k:
            for t in range(tiles):
                p0, p1, p2 = thirds(left[t] * scale[t])
                q0, q1, q2 = thirds(jnp.concatenate([left[t], right[t]], axis=1))
                p = jnp.concatenate([p0, p1, p0, p2, p0, p1], axis=0).astype(bf16)
                q = jnp.concatenate([q0, q0, q1, q0, q2, q1], axis=0).astype(bf16)
                update = mm(p, q, TN)
                work[t, top + b :, :] = work[t, top + b :, :] - update[top + b :, :]


def rows_loop(n, step, body):
    def one(i, carry):
        body(pl.ds(pl.multiple_of(i * step, step), step))
        return carry

    lax.fori_loop(0, n // step, one, 0)


def sketched(u_ref, v_ref, s_ref, out_ref):
    rhs = doubled_rows(product_tn(v_ref[0], s_ref[...]))

    def body(at):
        out_ref[0, at, :] = fold(mm(beside(u_ref[0, at, :]), rhs, NN))

    rows_loop(u_ref.shape[1], 512, body)


def sketch_tiles(tile_u, tile_v, sketch):
    tiles, n, k = tile_u.shape
    block = pl.BlockSpec((1, n, k), lambda i: (i, 0, 0))
    return pl.pallas_call(
        sketched,
        grid=(tiles,),
        in_specs=[block, block, pl.BlockSpec((n, k), lambda i: (0, 0))],
        out_specs=block,
        out_shape=jax.ShapeDtypeStruct(tile_u.shape, f32),
        cost_estimate=pl.CostEstimate(flops=6 * tiles * n * k * k * 2, bytes_accessed=12 * tiles * n * k, transcendentals=0),
        name="sketch_tiles",
    )(tile_u, tile_v, sketch)


def projected(v_ref, s_ref, out_ref):
    out_ref[0] = product_tn(v_ref[0], s_ref[...])


def project(v, sketch):
    tiles, n, k = v.shape
    return pl.pallas_call(
        projected,
        grid=(tiles,),
        in_specs=[pl.BlockSpec((1, n, k), lambda i: (i, 0, 0)), pl.BlockSpec((n, k), lambda i: (0, 0))],
        out_specs=pl.BlockSpec((1, k, k), lambda i: (i, 0, 0)),
        out_shape=jax.ShapeDtypeStruct((tiles, k, k), f32),
        cost_estimate=pl.CostEstimate(flops=6 * tiles * n * k * k, bytes_accessed=4 * tiles * n * k, transcendentals=0),
        name="project",
    )(v, sketch)


def recompress_kernel(tiles, n, k, cores, small, row_u, base, tile_u, tile_v, col_u, new_u, new_v,
                      s, tu, tv, cu, ru, work, cross, back, row_parts, sem):
    root = math.sqrt(n)
    copies = [pltpu.make_async_copy(row_u, ru, sem.at[0])]
    for t in range(tiles):
        copies.append(pltpu.make_async_copy(base.at[t], s.at[t], sem.at[1 + t]))
        copies.append(pltpu.make_async_copy(tile_u.at[t], tu.at[t], sem.at[1 + tiles + t]))
    late = []
    for t in range(tiles):
        late.append(pltpu.make_async_copy(tile_v.at[t], tv.at[t], sem.at[1 + 2 * tiles + t]))
        late.append(pltpu.make_async_copy(col_u.at[t], cu.at[t], sem.at[1 + 3 * tiles + t]))
    for c in copies + late:
        c.start()
    copies[0].wait()

    def split(at):
        row_parts[at, :] = beside(ru[at, :])

    rows_loop(n, 512, split)
    for t in range(tiles):
        copies[1 + 2 * t].wait()
        copies[2 + 2 * t].wait()
        rhs = doubled_rows(-product(cores[t], small[t]))

        def update(at, t=t, rhs=rhs):
            s[t, at, :] = s[t, at, :] + fold(mm(row_parts[at, :], rhs, NN))

        rows_loop(n, 512, update)
        work[t] = jnp.zeros((k, 2 * k), f32)
        cross[t] = jnp.zeros((k, 2 * k), f32)

        def gather(at, t=t):
            part = beside(s[t, at, :])
            x = mm(part, jnp.concatenate([part, beside(tu[t, at, :]), row_parts[at, :]], axis=1), TN)
            x = x[:k] + x[k:]
            work[t, :, :k] += fold(x[:, : 2 * k])
            cross[t, :, :k] += fold(x[:, 2 * k : 4 * k])
            cross[t, :, k:] += fold(x[:, 4 * k :])

        rows_loop(n, 512, gather)
    eye = jnp.where(
        lax.broadcasted_iota(jnp.int32, (k, k), 0) == lax.broadcasted_iota(jnp.int32, (k, k), 1), 1.0, 0.0
    ).astype(f32)
    for t in range(tiles):
        work[t, :, k:] = eye
    eliminate(work, tiles, k)
    outs = []
    for t in range(tiles):
        inverse = work[t, :, k:]
        y = product(inverse, cross[t]) * (1.0 / root)
        c1 = y[:, :k]
        c2 = -product(y[:, k:], cores[t])
        late[2 * t].wait()
        late[2 * t + 1].wait()
        by = doubled_columns(inverse * root)
        c12 = jnp.concatenate([doubled_columns(c1), doubled_columns(c2)], axis=1)

        def finish(at, t=t, by=by, c12=c12):
            s[t, at, :] = fold(mm(beside(s[t, at, :]), by, NT))
            lhs = jnp.concatenate([beside(tv[t, at, :]), beside(cu[t, at, :])], axis=1)
            tv[t, at, :] = fold(mm(lhs, c12, NT))

        rows_loop(n, 512, finish)
        outs.append(pltpu.make_async_copy(s.at[t], new_u.at[t], sem.at[1 + 4 * tiles + t]))
        outs.append(pltpu.make_async_copy(tv.at[t], new_v.at[t], sem.at[1 + 5 * tiles + t]))
        outs[-2].start()
        outs[-1].start()
    for c in outs:
        c.wait()


def recompress(cores, small, row_u, base, tile_u, tile_v, col_u):
    tiles, n, k = tile_u.shape
    any_ = pl.BlockSpec(memory_space=ANY)
    vmem = pl.BlockSpec(memory_space=VMEM)
    full = lambda: VMEM((tiles, n, k), f32)
    return pl.pallas_call(
        functools.partial(recompress_kernel, tiles, n, k),
        in_specs=[vmem, vmem] + [any_] * 5,
        out_specs=[any_, any_],
        out_shape=[jax.ShapeDtypeStruct(tile_u.shape, f32)] * 2,
        scratch_shapes=[
            full(), full(), full(), full(), VMEM((n, k), f32),
            VMEM((tiles, k, 2 * k), f32), VMEM((tiles, k, 2 * k), f32), VMEM((tiles, k, 2 * k), f32),
            VMEM((n, 2 * k), bf16),
            pltpu.SemaphoreType.DMA((1 + 6 * tiles,)),
        ],
        compiler_params=pltpu.CompilerParams(vmem_limit_bytes=40 * 1024 * 1024),
        cost_estimate=pl.CostEstimate(flops=24 * tiles * n * k * k, bytes_accessed=28 * tiles * n * k, transcendentals=0),
        name="recompress",
    )(cores, small, row_u, base, tile_u, tile_v, col_u)


highest = lax.Precision.HIGHEST


def body(tile_u, tile_v, row_panel_u, row_panel_v, col_panel_u, col_panel_v, diag_inverse, sketch):
    first = jnp.einsum(
        "ab,tbk->tak",
        diag_inverse,
        lax.all_gather(row_panel_v, "col", axis=1, tiled=True),
        precision=highest,
    )
    second = jnp.einsum(
        "ab,tbk->tak",
        diag_inverse,
        lax.all_gather(col_panel_v, "col", axis=1, tiled=True),
        precision=highest,
    )
    col_u_rows, col_v_rows = (
        lax.all_gather(col_panel_u, "row", axis=0, tiled=True),
        lax.all_gather(second, "row", axis=0, tiled=True),
    )
    row_u_full = lax.all_gather(row_panel_u, "col", axis=1, tiled=True)
    col_u_full = lax.all_to_all(col_u_rows, "col", split_axis=0, concat_axis=1, tiled=True)
    partial_cores = jnp.einsum("iak,jal->ijkl", first, col_v_rows, precision=highest)
    cores = lax.psum_scatter(partial_cores, "col", scatter_dimension=1, tiled=True)
    base = sketch_tiles(tile_u[0], tile_v[0], sketch)
    small = project(col_u_full, sketch)
    new_u, new_v = recompress(cores[0], small, row_u_full[0], base, tile_u[0], tile_v[0], col_u_full)
    return new_u[None], new_v[None]


def solution(mesh):
    in_specs = (
        P("row", "col", None, None),
        P("row", "col", None, None),
        P("row", "col", None),
        P("row", "col", None),
        P("row", "col", None),
        P("row", "col", None),
        P("col", None),
        P(),
    )
    out_specs = (P("row", "col", None, None), P("row", "col", None, None))
    return jax.shard_map(body, mesh=mesh, in_specs=in_specs, out_specs=out_specs, check_vma=False)
```

```python
import functools
import math

import jax
import jax.numpy as jnp
from jax import lax
from jax.experimental import pallas as pl
from jax.experimental.pallas import tpu as pltpu
from jax.sharding import PartitionSpec as P

f32, bf16 = jnp.float32, jnp.bfloat16
ANY, VMEM = pl.ANY, pltpu.VMEM
NT = (((1,), (1,)), ((), ()))
NN = (((1,), (0,)), ((), ()))
TN = (((0,), (0,)), ((), ()))


def mm(a, b, dims):
    return lax.dot_general(a, b, dims, preferred_element_type=f32)


def halves(x):
    hi = x.astype(bf16)
    return hi, (x - hi.astype(f32)).astype(bf16)


def beside(x):
    return jnp.concatenate(halves(x), axis=1)


def doubled_rows(x):
    both = beside(x)
    return jnp.concatenate([both, both], axis=0)


def doubled_columns(x):
    hi, lo = halves(x)
    return jnp.concatenate([jnp.concatenate([hi, hi], axis=1), jnp.concatenate([lo, lo], axis=1)], axis=0)


def fold(x):
    w = x.shape[1] // 2
    return x[:, :w] + x[:, w:]


def product(a, b):
    return fold(mm(beside(a), doubled_rows(b), NN))


def product_tn(a, b):
    x = fold(mm(beside(a), beside(b), TN))
    h = x.shape[0] // 2
    return x[:h] + x[h:]


def thirds(x):
    a = x.astype(bf16).astype(f32)
    r = x - a
    b = r.astype(bf16).astype(f32)
    return a, b, r - b


def eliminate(work, tiles, k):
    b = 8
    row = lax.broadcasted_iota(jnp.int32, (b, k), 0)
    for top in range(0, k, b):
        left, right, cols, scale = [], [], [], []
        for t in range(tiles):
            x = work[t, top : top + b, :]
            left.append(x[:, :k])
            right.append(x[:, k:])
            cols.append([jnp.broadcast_to(x[:, top + j : top + j + 1], (b, k)) for j in range(b)])
            scale.append(jnp.zeros((b, k), f32))
        for j in range(b):
            for t in range(tiles):
                pivot = jnp.broadcast_to(cols[t][j][j : j + 1, :], (b, k))
                inverse = 1.0 / pivot
                scale[t] = jnp.where(row == j, inverse, scale[t])
                if j + 1 < b:
                    m = jnp.where(row > j, cols[t][j] * inverse, 0.0)
                    for u in range(j + 1, b):
                        cols[t][u] = cols[t][u] - m * cols[t][u][j : j + 1, :]
                    left[t] = left[t] - m * left[t][j : j + 1, :]
                    right[t] = right[t] - m * right[t][j : j + 1, :]
        for t in range(tiles):
            work[t, top : top + b, k:] = right[t] * jnp.sqrt(scale[t])
        if top + b < k:
            for t in range(tiles):
                p0, p1, p2 = thirds(left[t] * scale[t])
                q0, q1, q2 = thirds(jnp.concatenate([left[t], right[t]], axis=1))
                p = jnp.concatenate([p0, p1, p0, p2, p0, p1], axis=0).astype(bf16)
                q = jnp.concatenate([q0, q0, q1, q0, q2, q1], axis=0).astype(bf16)
                update = mm(p, q, TN)
                work[t, top + b :, :] = work[t, top + b :, :] - update[top + b :, :]


def rows_loop(n, step, body):
    def one(i, carry):
        body(pl.ds(pl.multiple_of(i * step, step), step))
        return carry

    lax.fori_loop(0, n // step, one, 0)


def sketched(u_ref, v_ref, s_ref, out_ref):
    rhs = doubled_rows(product_tn(v_ref[0], s_ref[...]))

    def body(at):
        out_ref[0, at, :] = fold(mm(beside(u_ref[0, at, :]), rhs, NN))

    rows_loop(u_ref.shape[1], 512, body)


def sketch_tiles(tile_u, tile_v, sketch):
    tiles, n, k = tile_u.shape
    block = pl.BlockSpec((1, n, k), lambda i: (i, 0, 0))
    return pl.pallas_call(
        sketched,
        grid=(tiles,),
        in_specs=[block, block, pl.BlockSpec((n, k), lambda i: (0, 0))],
        out_specs=block,
        out_shape=jax.ShapeDtypeStruct(tile_u.shape, f32),
        cost_estimate=pl.CostEstimate(flops=6 * tiles * n * k * k * 2, bytes_accessed=12 * tiles * n * k, transcendentals=0),
        name="sketch_tiles",
    )(tile_u, tile_v, sketch)


def block_of(c, d, n):
    return lax.rem(c - d + n, n)


def project_kernel(n_col, at, mine, other, s_ref, full, small):
    r, c = at[0], at[1]
    chip, core = lax.shift_right_logical(r, 1), lax.rem(r, 2)
    chips, _, pair, piece, _ = mine.shape
    for src, parity in ((mine, core), (other, 1 - core)):
        for e in range(chips):
            for d in range(n_col):
                start = block_of(c, d, n_col) * (chips * piece) + (chip ^ e) * piece
                rows = pl.ds(pl.multiple_of(start, piece), piece)
                for t in range(pair):
                    full[parity * pair + t, rows, :] = src[e, d, t]
    for j in range(full.shape[0]):
        small[j] = product_tn(full[j], s_ref[...])


def project(n_col, at, mine, other, sketch):
    chips, _, pair, piece, k = mine.shape
    tiles, n = 2 * pair, chips * n_col * piece
    vmem = pl.BlockSpec(memory_space=VMEM)
    return pl.pallas_call(
        functools.partial(project_kernel, n_col),
        in_specs=[pl.BlockSpec(memory_space=pltpu.SMEM)] + [vmem] * 3,
        out_specs=[vmem] * 2,
        out_shape=[jax.ShapeDtypeStruct((tiles, n, k), f32), jax.ShapeDtypeStruct((tiles, k, k), f32)],
        cost_estimate=pl.CostEstimate(flops=6 * tiles * n * k * k, bytes_accessed=8 * tiles * n * k, transcendentals=0),
        name="project",
    )(at, mine, other, sketch)


def solve_kernel(n_col, at, diag, *refs):
    xs, outs = refs[:n_col], refs[n_col:]
    c = at[1]
    rows = diag.shape[0]
    solved = None
    for d in range(n_col):
        cols = pl.ds(pl.multiple_of(jnp.maximum(c - d, 0) * rows, rows), rows)
        part = product(diag[:, cols], xs[d][...])
        solved = part if solved is None else solved + part
    for d in range(n_col):
        cols = pl.ds(pl.multiple_of(jnp.maximum(c - d, 0) * rows, rows), rows)
        outs[d][...] = product_tn(solved, diag[:, cols])


def solve(at, diag, xs):
    n_col = len(xs)
    rows, k = xs[0].shape
    vmem = pl.BlockSpec(memory_space=VMEM)
    return pl.pallas_call(
        functools.partial(solve_kernel, n_col),
        in_specs=[pl.BlockSpec(memory_space=pltpu.SMEM)] + [vmem] * (1 + n_col),
        out_specs=[vmem] * n_col,
        out_shape=[jax.ShapeDtypeStruct((k, rows), f32)] * n_col,
        cost_estimate=pl.CostEstimate(flops=12 * n_col * rows * rows * k, bytes_accessed=4 * n_col * rows * rows, transcendentals=0),
        name="solve",
    )(at, diag, *xs)


def cores_kernel(n_col, at, *refs):
    parts, (mine, other), outs = refs[:n_col], refs[n_col : n_col + 2], refs[n_col + 2 :]
    r, c = at[0], at[1]
    chip, core = lax.shift_right_logical(r, 1), lax.rem(r, 2)
    total = parts[0][...]
    for p in parts[1:]:
        total = total + p[...]
    lhs = beside(total)
    pair = mine.shape[1]
    for d in range(n_col):
        e = chip ^ lax.rem(c + d, n_col)
        for src, parity in ((mine, core), (other, 1 - core)):
            for t in range(pair):
                outs[d][parity * pair + t] = fold(mm(lhs, doubled_rows(src[e, t]), NN))


def partial_cores(at, parts, mine, other):
    n_col = len(parts)
    k, rows = parts[0].shape
    pair = mine.shape[1]
    vmem = pl.BlockSpec(memory_space=VMEM)
    return pl.pallas_call(
        functools.partial(cores_kernel, n_col),
        in_specs=[pl.BlockSpec(memory_space=pltpu.SMEM)] + [vmem] * (n_col + 2),
        out_specs=[vmem] * n_col,
        out_shape=[jax.ShapeDtypeStruct((2 * pair, k, k), f32)] * n_col,
        cost_estimate=pl.CostEstimate(flops=12 * n_col * pair * rows * k * k, bytes_accessed=8 * n_col * pair * rows * k, transcendentals=0),
        name="partial_cores",
    )(at, *parts, mine, other)


def recompress_kernel(tiles, n, k, n_col, at, *refs):
    core_parts, row_us = refs[:n_col], refs[n_col : 2 * n_col]
    small, base, tile_u, tile_v, col_u, new_u, new_v = refs[2 * n_col : 2 * n_col + 7]
    s, tu, tv, cu, ru, work, cross, cores, row_parts, sem, row_sem = refs[2 * n_col + 7 :]
    c = at[1]
    root = math.sqrt(n)
    blk = n // n_col
    row_copies = []
    for d in range(n_col):
        rows = pl.ds(pl.multiple_of(block_of(c, d, n_col) * blk, blk), blk)
        row_copies.append(pltpu.make_async_copy(row_us[d], ru.at[rows], row_sem.at[d]))
    copies = []
    for t in range(tiles):
        copies.append(pltpu.make_async_copy(base.at[t], s.at[t], sem.at[t]))
        copies.append(pltpu.make_async_copy(tile_u.at[t], tu.at[t], sem.at[tiles + t]))
    late = []
    for t in range(tiles):
        late.append(pltpu.make_async_copy(tile_v.at[t], tv.at[t], sem.at[2 * tiles + t]))
        late.append(pltpu.make_async_copy(col_u.at[t], cu.at[t], sem.at[3 * tiles + t]))
    for x in row_copies + copies + late:
        x.start()
    total = core_parts[0][...]
    for p in core_parts[1:]:
        total = total + p[...]
    cores[...] = total
    for x in row_copies:
        x.wait()

    def split(at):
        row_parts[at, :] = beside(ru[at, :])

    rows_loop(n, 512, split)
    for t in range(tiles):
        copies[2 * t].wait()
        copies[2 * t + 1].wait()
        rhs = doubled_rows(-product(cores[t], small[t]))

        def update(at, t=t, rhs=rhs):
            s[t, at, :] = s[t, at, :] + fold(mm(row_parts[at, :], rhs, NN))

        rows_loop(n, 512, update)
        work[t] = jnp.zeros((k, 2 * k), f32)
        cross[t] = jnp.zeros((k, 2 * k), f32)

        def gather(at, t=t):
            part = beside(s[t, at, :])
            x = mm(part, jnp.concatenate([part, beside(tu[t, at, :]), row_parts[at, :]], axis=1), TN)
            x = x[:k] + x[k:]
            work[t, :, :k] += fold(x[:, : 2 * k])
            cross[t, :, :k] += fold(x[:, 2 * k : 4 * k])
            cross[t, :, k:] += fold(x[:, 4 * k :])

        rows_loop(n, 512, gather)
    eye = jnp.where(
        lax.broadcasted_iota(jnp.int32, (k, k), 0) == lax.broadcasted_iota(jnp.int32, (k, k), 1), 1.0, 0.0
    ).astype(f32)
    for t in range(tiles):
        work[t, :, k:] = eye
    eliminate(work, tiles, k)
    outs = []
    for t in range(tiles):
        inverse = work[t, :, k:]
        y = product(inverse, cross[t]) * (1.0 / root)
        c1 = y[:, :k]
        c2 = -product(y[:, k:], cores[t])
        late[2 * t].wait()
        late[2 * t + 1].wait()
        by = doubled_columns(inverse * root)
        c12 = jnp.concatenate([doubled_columns(c1), doubled_columns(c2)], axis=1)

        def finish(at, t=t, by=by, c12=c12):
            s[t, at, :] = fold(mm(beside(s[t, at, :]), by, NT))
            lhs = jnp.concatenate([beside(tv[t, at, :]), beside(cu[t, at, :])], axis=1)
            tv[t, at, :] = fold(mm(lhs, c12, NT))

        rows_loop(n, 512, finish)
        outs.append(pltpu.make_async_copy(s.at[t], new_u.at[t], sem.at[4 * tiles + t]))
        outs.append(pltpu.make_async_copy(tv.at[t], new_v.at[t], sem.at[5 * tiles + t]))
        outs[-2].start()
        outs[-1].start()
    for x in outs:
        x.wait()


def recompress(at, core_parts, row_us, small, base, tile_u, tile_v, col_u):
    tiles, n, k = tile_u.shape
    n_col = len(core_parts)
    any_ = pl.BlockSpec(memory_space=ANY)
    vmem = pl.BlockSpec(memory_space=VMEM)
    full = lambda: VMEM((tiles, n, k), f32)
    return pl.pallas_call(
        functools.partial(recompress_kernel, tiles, n, k, n_col),
        in_specs=[pl.BlockSpec(memory_space=pltpu.SMEM)] + [vmem] * n_col + [any_] * n_col + [vmem] + [any_] * 4,
        out_specs=[any_, any_],
        out_shape=[jax.ShapeDtypeStruct(tile_u.shape, f32)] * 2,
        scratch_shapes=[
            full(), full(), full(), full(), VMEM((n, k), f32),
            VMEM((tiles, k, 2 * k), f32), VMEM((tiles, k, 2 * k), f32), VMEM((tiles, k, k), f32),
            VMEM((n, 2 * k), bf16),
            pltpu.SemaphoreType.DMA((6 * tiles,)), pltpu.SemaphoreType.DMA((n_col,)),
        ],
        cost_estimate=pl.CostEstimate(flops=24 * tiles * n * k * k, bytes_accessed=28 * tiles * n * k, transcendentals=0),
        name="recompress",
    )(at, *core_parts, *row_us, small, base, tile_u, tile_v, col_u)


def step(n_row, n_col, tile_u, tile_v, row_panel_u, row_panel_v, col_panel_u, col_panel_v, diag_inverse, sketch):
    chips = n_row // 2
    r, c = lax.axis_index("row"), lax.axis_index("col")
    at = jnp.stack([r, c]).astype(jnp.int32)
    chip = lax.shift_right_logical(r, 1)

    def partner(x, m):
        return lax.ppermute(x, "row", [(a, a ^ m) for a in range(n_row)])

    def shift(x, pairs):
        return lax.ppermute(x, "col", pairs)

    def up(x, d):
        return shift(x, [(a, a + d) for a in range(n_col - d)])

    def down(x, d):
        return shift(x, [(a, a - d) for a in range(d, n_col)])

    def around(x, d):
        return shift(x, [(a, (a + d) % n_col) for a in range(n_col)])

    def pick(x, i, axis=0):
        return lax.dynamic_index_in_dim(x, i, axis, keepdims=False)

    row_v = row_panel_v[0]
    below = [row_v] + [up(row_v, d) for d in range(1, n_col)]
    col_v_mine = jnp.stack([col_panel_v] + [partner(col_panel_v, 2 * e) for e in range(1, chips)])
    row_u = row_panel_u[0]
    row_us = [row_u] + [around(row_u, d) for d in range(1, n_col)]
    pair, rows, k = col_panel_u.shape
    cut = col_panel_u.reshape(pair, chips, rows // chips, k)
    cuts = jnp.stack([pick(cut, chip, 1)] + [partner(pick(cut, chip ^ e, 1), 2 * e) for e in range(1, chips)])
    col_v_other = partner(col_v_mine, 1)
    planes = jnp.stack(
        [pick(cuts, chip ^ c)] + [around(pick(cuts, chip ^ lax.rem(c + d, n_col)), d) for d in range(1, n_col)]
    )
    base = sketch_tiles(tile_u[0], tile_v[0], sketch)
    sums = solve(at, diag_inverse, below)
    parts = [sums[0]] + [down(sums[d], d) for d in range(1, n_col)]
    gathered = [planes] + [partner(planes, 2 * e) for e in range(1, chips)]
    col_u_mine = jnp.stack(gathered)
    col_u_other = partner(col_u_mine, 1)
    col_u, small = project(n_col, at, col_u_mine, col_u_other, sketch)
    cores = partial_cores(at, parts, col_v_mine, col_v_other)
    core_parts = [cores[0]] + [around(cores[d], d) for d in range(1, n_col)]
    new_u, new_v = recompress(at, core_parts, row_us, small, base, tile_u[0], tile_v[0], col_u)
    return new_u[None], new_v[None]


def solution(mesh):
    n_row, n_col = mesh.shape["row"], mesh.shape["col"]
    in_specs = (
        P("row", "col", None, None),
        P("row", "col", None, None),
        P("row", "col", None),
        P("row", "col", None),
        P("row", "col", None),
        P("row", "col", None),
        P("col", None),
        P(),
    )
    out_specs = (P("row", "col", None, None), P("row", "col", None, None))

    def body(*args):
        return step(n_row, n_col, *args)

    return jax.shard_map(body, mesh=mesh, in_specs=in_specs, out_specs=out_specs, check_vma=False)
```

```python
import functools
import math

import jax
import jax.numpy as jnp
from jax import lax
from jax.experimental import pallas as pl
from jax.experimental.pallas import tpu as pltpu
from jax.sharding import PartitionSpec as P

f32, bf16 = jnp.float32, jnp.bfloat16
ANY, VMEM = pl.ANY, pltpu.VMEM
NT = (((1,), (1,)), ((), ()))
NN = (((1,), (0,)), ((), ()))
TN = (((0,), (0,)), ((), ()))


def mm(a, b, dims):
    return lax.dot_general(a, b, dims, preferred_element_type=f32)


def halves(x):
    hi = x.astype(bf16)
    return hi, (x - hi.astype(f32)).astype(bf16)


def beside(x):
    return jnp.concatenate(halves(x), axis=1)


def doubled_rows(x):
    both = beside(x)
    return jnp.concatenate([both, both], axis=0)


def doubled_columns(x):
    hi, lo = halves(x)
    return jnp.concatenate([jnp.concatenate([hi, hi], axis=1), jnp.concatenate([lo, lo], axis=1)], axis=0)


def fold(x):
    w = x.shape[1] // 2
    return x[:, :w] + x[:, w:]


def product(a, b):
    return fold(mm(beside(a), doubled_rows(b), NN))


def product_tn(a, b):
    x = fold(mm(beside(a), beside(b), TN))
    h = x.shape[0] // 2
    return x[:h] + x[h:]


def thirds(x):
    a = x.astype(bf16).astype(f32)
    r = x - a
    b = r.astype(bf16).astype(f32)
    return a, b, r - b


def eliminate(work, tiles, k):
    b = 8
    row = lax.broadcasted_iota(jnp.int32, (b, k), 0)
    for top in range(0, k, b):
        left, right, cols, scale = [], [], [], []
        for t in range(tiles):
            x = work[t, top : top + b, :]
            left.append(x[:, :k])
            right.append(x[:, k:])
            cols.append([jnp.broadcast_to(x[:, top + j : top + j + 1], (b, k)) for j in range(b)])
            scale.append(jnp.zeros((b, k), f32))
        for j in range(b):
            for t in range(tiles):
                pivot = jnp.broadcast_to(cols[t][j][j : j + 1, :], (b, k))
                inverse = 1.0 / pivot
                scale[t] = jnp.where(row == j, inverse, scale[t])
                if j + 1 < b:
                    m = jnp.where(row > j, cols[t][j] * inverse, 0.0)
                    for u in range(j + 1, b):
                        cols[t][u] = cols[t][u] - m * cols[t][u][j : j + 1, :]
                    left[t] = left[t] - m * left[t][j : j + 1, :]
                    right[t] = right[t] - m * right[t][j : j + 1, :]
        for t in range(tiles):
            work[t, top : top + b, k:] = right[t] * jnp.sqrt(scale[t])
        if top + b < k:
            for t in range(tiles):
                p0, p1, p2 = thirds(left[t] * scale[t])
                q0, q1, q2 = thirds(jnp.concatenate([left[t], right[t]], axis=1))
                p = jnp.concatenate([p0, p1, p0, p2, p0, p1], axis=0).astype(bf16)
                q = jnp.concatenate([q0, q0, q1, q0, q2, q1], axis=0).astype(bf16)
                update = mm(p, q, TN)
                work[t, top + b :, :] = work[t, top + b :, :] - update[top + b :, :]


def rows_loop(n, step, body):
    def one(i, carry):
        body(pl.ds(pl.multiple_of(i * step, step), step))
        return carry

    lax.fori_loop(0, n // step, one, 0)


def sketched(u_ref, v_ref, s_ref, out_ref, u_parts, v_parts):
    v = beside(v_ref[0])
    v_parts[0] = v
    x = fold(mm(v, beside(s_ref[...]), TN))
    h = x.shape[0] // 2
    rhs = doubled_rows(x[:h] + x[h:])

    def body(at):
        u = beside(u_ref[0, at, :])
        u_parts[0, at, :] = u
        out_ref[0, at, :] = fold(mm(u, rhs, NN))

    rows_loop(u_ref.shape[1], 512, body)


def sketch_tiles(tile_u, tile_v, sketch):
    tiles, n, k = tile_u.shape
    block = pl.BlockSpec((1, n, k), lambda i: (i, 0, 0))
    parts = pl.BlockSpec((1, n, 2 * k), lambda i: (i, 0, 0))
    return pl.pallas_call(
        sketched,
        grid=(tiles,),
        in_specs=[block, block, pl.BlockSpec((n, k), lambda i: (0, 0))],
        out_specs=[block, parts, parts],
        out_shape=[jax.ShapeDtypeStruct(tile_u.shape, f32)] + [jax.ShapeDtypeStruct((tiles, n, 2 * k), bf16)] * 2,
        cost_estimate=pl.CostEstimate(flops=6 * tiles * n * k * k * 2, bytes_accessed=20 * tiles * n * k, transcendentals=0),
        name="sketch_tiles",
    )(tile_u, tile_v, sketch)


def block_of(c, d, n):
    return lax.rem(c - d + n, n)


def project_kernel(n_col, at, mine, other, s_ref, full, small):
    r, c = at[0], at[1]
    chip, core = lax.shift_right_logical(r, 1), lax.rem(r, 2)
    chips, _, pair, piece, _ = mine.shape
    for src, parity in ((mine, core), (other, 1 - core)):
        for e in range(chips):
            for d in range(n_col):
                start = block_of(c, d, n_col) * (chips * piece) + (chip ^ e) * piece
                rows = pl.ds(pl.multiple_of(start, piece), piece)
                for t in range(pair):
                    full[parity * pair + t, rows, :] = beside(src[e, d, t])
    rhs = beside(s_ref[...])
    for j in range(full.shape[0]):
        x = fold(mm(full[j], rhs, TN))
        h = x.shape[0] // 2
        small[j] = x[:h] + x[h:]


def project(n_col, at, mine, other, sketch):
    chips, _, pair, piece, k = mine.shape
    tiles, n = 2 * pair, chips * n_col * piece
    vmem = pl.BlockSpec(memory_space=VMEM)
    return pl.pallas_call(
        functools.partial(project_kernel, n_col),
        in_specs=[pl.BlockSpec(memory_space=pltpu.SMEM)] + [vmem] * 3,
        out_specs=[vmem] * 2,
        out_shape=[jax.ShapeDtypeStruct((tiles, n, 2 * k), bf16), jax.ShapeDtypeStruct((tiles, k, k), f32)],
        cost_estimate=pl.CostEstimate(flops=6 * tiles * n * k * k, bytes_accessed=8 * tiles * n * k, transcendentals=0),
        name="project",
    )(at, mine, other, sketch)


def solve_kernel(n_col, at, diag, *refs):
    xs, outs = refs[:n_col], refs[n_col:]
    c = at[1]
    rows = diag.shape[0]
    solved = None
    for d in range(n_col):
        cols = pl.ds(pl.multiple_of(jnp.maximum(c - d, 0) * rows, rows), rows)
        part = product(diag[:, cols], xs[d][...])
        solved = part if solved is None else solved + part
    for d in range(n_col):
        cols = pl.ds(pl.multiple_of(jnp.maximum(c - d, 0) * rows, rows), rows)
        outs[d][...] = product_tn(solved, diag[:, cols])


def solve(at, diag, xs):
    n_col = len(xs)
    rows, k = xs[0].shape
    vmem = pl.BlockSpec(memory_space=VMEM)
    return pl.pallas_call(
        functools.partial(solve_kernel, n_col),
        in_specs=[pl.BlockSpec(memory_space=pltpu.SMEM)] + [vmem] * (1 + n_col),
        out_specs=[vmem] * n_col,
        out_shape=[jax.ShapeDtypeStruct((k, rows), f32)] * n_col,
        cost_estimate=pl.CostEstimate(flops=12 * n_col * rows * rows * k, bytes_accessed=4 * n_col * rows * rows, transcendentals=0),
        name="solve",
    )(at, diag, *xs)


def cores_kernel(n_col, at, *refs):
    parts, (mine, other), outs = refs[:n_col], refs[n_col : n_col + 2], refs[n_col + 2 :]
    r, c = at[0], at[1]
    chip, core = lax.shift_right_logical(r, 1), lax.rem(r, 2)
    total = parts[0][...]
    for p in parts[1:]:
        total = total + p[...]
    lhs = beside(total)
    pair = mine.shape[1]
    for d in range(n_col):
        e = chip ^ lax.rem(c + d, n_col)
        for src, parity in ((mine, core), (other, 1 - core)):
            for t in range(pair):
                outs[d][parity * pair + t] = fold(mm(lhs, doubled_rows(src[e, t]), NN))


def partial_cores(at, parts, mine, other):
    n_col = len(parts)
    k, rows = parts[0].shape
    pair = mine.shape[1]
    vmem = pl.BlockSpec(memory_space=VMEM)
    return pl.pallas_call(
        functools.partial(cores_kernel, n_col),
        in_specs=[pl.BlockSpec(memory_space=pltpu.SMEM)] + [vmem] * (n_col + 2),
        out_specs=[vmem] * n_col,
        out_shape=[jax.ShapeDtypeStruct((2 * pair, k, k), f32)] * n_col,
        cost_estimate=pl.CostEstimate(flops=12 * n_col * pair * rows * k * k, bytes_accessed=8 * n_col * pair * rows * k, transcendentals=0),
        name="partial_cores",
    )(at, *parts, mine, other)


def recompress_kernel(tiles, n, k, n_col, at, *refs):
    core_parts, row_us = refs[:n_col], refs[n_col : 2 * n_col]
    small, base, u_parts, v_parts, w_parts, new_u, new_v = refs[2 * n_col : 2 * n_col + 7]
    s, tu, tv, cu, sp, out, ru, work, cross, cores, row_parts, sem, row_sem = refs[2 * n_col + 7 :]
    c = at[1]
    root = math.sqrt(n)
    blk = n // n_col
    row_copies = []
    for d in range(n_col):
        rows = pl.ds(pl.multiple_of(block_of(c, d, n_col) * blk, blk), blk)
        row_copies.append(pltpu.make_async_copy(row_us[d], ru.at[rows], row_sem.at[d]))
    early, late, outs = [], [], []
    for t in range(tiles):
        early.append((
            pltpu.make_async_copy(base.at[t], s.at[t], sem.at[t]),
            pltpu.make_async_copy(u_parts.at[t], tu.at[t], sem.at[tiles + t]),
        ))
        late.append((
            pltpu.make_async_copy(v_parts.at[t], tv.at[t], sem.at[2 * tiles + t]),
            pltpu.make_async_copy(w_parts.at[t], cu.at[t], sem.at[3 * tiles + t]),
        ))
        outs.append((
            pltpu.make_async_copy(s.at[t], new_u.at[t], sem.at[4 * tiles + t]),
            pltpu.make_async_copy(out.at[t], new_v.at[t], sem.at[5 * tiles + t]),
        ))
    for x in row_copies:
        x.start()
    for x in early[0] + early[1]:
        x.start()
    total = core_parts[0][...]
    for p in core_parts[1:]:
        total = total + p[...]
    cores[...] = total
    for x in row_copies:
        x.wait()

    def split(at):
        row_parts[at, :] = beside(ru[at, :])

    rows_loop(n, 512, split)
    for t in range(tiles):
        for x in early[t]:
            x.wait()
        for x in (early + late)[t + 2]:
            x.start()
        rhs = doubled_rows(-product(cores[t], small[t]))
        work[t] = jnp.zeros((k, 2 * k), f32)
        cross[t] = jnp.zeros((k, 2 * k), f32)

        def gather(at, t=t, rhs=rhs):
            part = beside(s[t, at, :] + fold(mm(row_parts[at, :], rhs, NN)))
            sp[t, at, :] = part
            x = mm(part, jnp.concatenate([part, tu[t, at, :], row_parts[at, :]], axis=1), TN)
            x = x[:k] + x[k:]
            work[t, :, :k] += fold(x[:, : 2 * k])
            cross[t, :, :k] += fold(x[:, 2 * k : 4 * k])
            cross[t, :, k:] += fold(x[:, 4 * k :])

        gather(pl.ds(0, n))
    for pair in late[2:]:
        for x in pair:
            x.start()
    eye = jnp.where(
        lax.broadcasted_iota(jnp.int32, (k, k), 0) == lax.broadcasted_iota(jnp.int32, (k, k), 1), 1.0, 0.0
    ).astype(f32)
    for t in range(tiles):
        work[t, :, k:] = eye
    eliminate(work, tiles, k)
    for t in range(tiles):
        inverse = work[t, :, k:]
        y = product(inverse, cross[t]) * (1.0 / root)
        c1 = y[:, :k]
        c2 = -product(y[:, k:], cores[t])
        by = doubled_columns(inverse * root)
        c12 = jnp.concatenate([doubled_columns(c1), doubled_columns(c2)], axis=1)
        for x in late[t]:
            x.wait()

        def finish(at, t=t, by=by, c12=c12):
            s[t, at, :] = fold(mm(sp[t, at, :], by, NT))
            lhs = jnp.concatenate([tv[t, at, :], cu[t, at, :]], axis=1)
            out[t, at, :] = fold(mm(lhs, c12, NT))

        finish(pl.ds(0, n))
        for x in outs[t]:
            x.start()
    for pair in outs:
        for x in pair:
            x.wait()


def recompress(at, core_parts, row_us, small, base, u_parts, v_parts, w_parts):
    tiles, n, k = base.shape
    n_col = len(core_parts)
    any_ = pl.BlockSpec(memory_space=ANY)
    vmem = pl.BlockSpec(memory_space=VMEM)
    full = lambda: VMEM((tiles, n, k), f32)
    split = lambda: VMEM((tiles, n, 2 * k), bf16)
    return pl.pallas_call(
        functools.partial(recompress_kernel, tiles, n, k, n_col),
        in_specs=[pl.BlockSpec(memory_space=pltpu.SMEM)] + [vmem] * n_col + [any_] * n_col + [vmem] + [any_] * 4,
        out_specs=[any_, any_],
        out_shape=[jax.ShapeDtypeStruct(base.shape, f32)] * 2,
        scratch_shapes=[
            full(), split(), split(), split(), split(), full(), VMEM((n, k), f32),
            VMEM((tiles, k, 2 * k), f32), VMEM((tiles, k, 2 * k), f32), VMEM((tiles, k, k), f32),
            VMEM((n, 2 * k), bf16),
            pltpu.SemaphoreType.DMA((6 * tiles,)), pltpu.SemaphoreType.DMA((n_col,)),
        ],
        cost_estimate=pl.CostEstimate(flops=24 * tiles * n * k * k, bytes_accessed=28 * tiles * n * k, transcendentals=0),
        name="recompress",
    )(at, *core_parts, *row_us, small, base, u_parts, v_parts, w_parts)


def step(n_row, n_col, tile_u, tile_v, row_panel_u, row_panel_v, col_panel_u, col_panel_v, diag_inverse, sketch):
    chips = n_row // 2
    r, c = lax.axis_index("row"), lax.axis_index("col")
    at = jnp.stack([r, c]).astype(jnp.int32)
    chip = lax.shift_right_logical(r, 1)

    def partner(x, m):
        return lax.ppermute(x, "row", [(a, a ^ m) for a in range(n_row)])

    def shift(x, pairs):
        return lax.ppermute(x, "col", pairs)

    def up(x, d):
        return shift(x, [(a, a + d) for a in range(n_col - d)])

    def down(x, d):
        return shift(x, [(a, a - d) for a in range(d, n_col)])

    def around(x, d):
        return shift(x, [(a, (a + d) % n_col) for a in range(n_col)])

    def pick(x, i, axis=0):
        return lax.dynamic_index_in_dim(x, i, axis, keepdims=False)

    row_v = row_panel_v[0]
    below = [row_v] + [up(row_v, d) for d in range(1, n_col)]
    col_v_mine = jnp.stack([col_panel_v] + [partner(col_panel_v, 2 * e) for e in range(1, chips)])
    row_u = row_panel_u[0]
    rises = [up(row_u, d) for d in range(1, n_col)]
    falls = [down(row_u, d) for d in range(1, n_col)]
    row_us = [row_u] + [jnp.where(c >= d, rises[d - 1], falls[n_col - d - 1]) for d in range(1, n_col)]
    pair, rows, k = col_panel_u.shape
    cut = col_panel_u.reshape(pair, chips, rows // chips, k)
    cuts = jnp.stack([pick(cut, chip, 1)] + [partner(pick(cut, chip ^ e, 1), 2 * e) for e in range(1, chips)])
    col_v_other = partner(col_v_mine, 1)
    moved = [pick(cuts, chip ^ c)] + [around(pick(cuts, chip ^ lax.rem(c + d, n_col)), d) for d in range(1, n_col)]
    planes = lax.optimization_barrier(jnp.stack(moved))
    base, u_parts, v_parts = sketch_tiles(tile_u[0], tile_v[0], sketch)
    sums = solve(at, diag_inverse, below)
    parts = [sums[0]] + [down(sums[d], d) for d in range(1, n_col)]
    gathered = [planes] + [partner(planes, 2 * e) for e in range(1, chips)]
    col_u_mine = jnp.stack(gathered)
    col_u_other = partner(col_u_mine, 1)
    w_parts, small = project(n_col, at, col_u_mine, col_u_other, sketch)
    cores = partial_cores(at, parts, col_v_mine, col_v_other)
    core_parts = [cores[0]] + [around(cores[d], d) for d in range(1, n_col)]
    new_u, new_v = recompress(at, core_parts, row_us, small, base, u_parts, v_parts, w_parts)
    return new_u[None], new_v[None]


def solution(mesh):
    n_row, n_col = mesh.shape["row"], mesh.shape["col"]
    in_specs = (
        P("row", "col", None, None),
        P("row", "col", None, None),
        P("row", "col", None),
        P("row", "col", None),
        P("row", "col", None),
        P("row", "col", None),
        P("col", None),
        P(),
    )
    out_specs = (P("row", "col", None, None), P("row", "col", None, None))

    def body(*args):
        return step(n_row, n_col, *args)

    return jax.shard_map(body, mesh=mesh, in_specs=in_specs, out_specs=out_specs, check_vma=False)
```

```python
import functools
import math

import jax
import jax.numpy as jnp
from jax import lax
from jax.experimental import pallas as pl
from jax.experimental.pallas import tpu as pltpu
from jax.sharding import PartitionSpec as P

f32, bf16 = jnp.float32, jnp.bfloat16
ANY, VMEM = pl.ANY, pltpu.VMEM
NT = (((1,), (1,)), ((), ()))
NN = (((1,), (0,)), ((), ()))
TN = (((0,), (0,)), ((), ()))


def mm(a, b, dims):
    return lax.dot_general(a, b, dims, preferred_element_type=f32)


def halves(x):
    hi = x.astype(bf16)
    return hi, (x - hi.astype(f32)).astype(bf16)


def beside(x):
    return jnp.concatenate(halves(x), axis=1)


def doubled_rows(x):
    both = beside(x)
    return jnp.concatenate([both, both], axis=0)


def doubled_columns(x):
    hi, lo = halves(x)
    return jnp.concatenate([jnp.concatenate([hi, hi], axis=1), jnp.concatenate([lo, lo], axis=1)], axis=0)


def fold(x):
    w = x.shape[1] // 2
    return x[:, :w] + x[:, w:]


def product(a, b):
    return fold(mm(beside(a), doubled_rows(b), NN))


def product_tn(a, b):
    x = fold(mm(beside(a), beside(b), TN))
    h = x.shape[0] // 2
    return x[:h] + x[h:]


def thirds(x):
    a = x.astype(bf16).astype(f32)
    r = x - a
    b = r.astype(bf16).astype(f32)
    return a, b, r - b


def eliminate(work, tiles, k):
    b = 8
    row = lax.broadcasted_iota(jnp.int32, (b, k), 0)
    for top in range(0, k, b):
        left, right, cols, scale = [], [], [], []
        for t in range(tiles):
            x = work[t, top : top + b, :]
            left.append(x[:, :k])
            right.append(x[:, k:])
            cols.append([jnp.broadcast_to(x[:, top + j : top + j + 1], (b, k)) for j in range(b)])
            scale.append(jnp.zeros((b, k), f32))
        for j in range(b):
            for t in range(tiles):
                pivot = jnp.broadcast_to(cols[t][j][j : j + 1, :], (b, k))
                inverse = 1.0 / pivot
                scale[t] = jnp.where(row == j, inverse, scale[t])
                if j + 1 < b:
                    m = jnp.where(row > j, cols[t][j] * inverse, 0.0)
                    for u in range(j + 1, b):
                        cols[t][u] = cols[t][u] - m * cols[t][u][j : j + 1, :]
                    left[t] = left[t] - m * left[t][j : j + 1, :]
                    right[t] = right[t] - m * right[t][j : j + 1, :]
        for t in range(tiles):
            work[t, top : top + b, k:] = right[t] * jnp.sqrt(scale[t])
        if top + b < k:
            for t in range(tiles):
                p0, p1, p2 = thirds(left[t] * scale[t])
                q0, q1, q2 = thirds(jnp.concatenate([left[t], right[t]], axis=1))
                p = jnp.concatenate([p0, p1, p0, p2, p0, p1], axis=0).astype(bf16)
                q = jnp.concatenate([q0, q0, q1, q0, q2, q1], axis=0).astype(bf16)
                update = mm(p, q, TN)
                work[t, top + b :, :] = work[t, top + b :, :] - update[top + b :, :]


def rows_loop(n, step, body):
    def one(i, carry):
        body(pl.ds(pl.multiple_of(i * step, step), step))
        return carry

    lax.fori_loop(0, n // step, one, 0)


def sketched(u_ref, v_ref, s_ref, out_ref, u_parts, v_parts):
    v = beside(v_ref[0])
    v_parts[0] = v
    x = fold(mm(v, beside(s_ref[...]), TN))
    h = x.shape[0] // 2
    rhs = doubled_rows(x[:h] + x[h:])

    def body(at):
        u = beside(u_ref[0, at, :])
        u_parts[0, at, :] = u
        out_ref[0, at, :] = fold(mm(u, rhs, NN))

    rows_loop(u_ref.shape[1], 512, body)


def sketch_tiles(tile_u, tile_v, sketch):
    tiles, n, k = tile_u.shape
    block = pl.BlockSpec((1, n, k), lambda i: (i, 0, 0))
    parts = pl.BlockSpec((1, n, 2 * k), lambda i: (i, 0, 0))
    return pl.pallas_call(
        sketched,
        grid=(tiles,),
        in_specs=[block, block, pl.BlockSpec((n, k), lambda i: (0, 0))],
        out_specs=[block, parts, parts],
        out_shape=[jax.ShapeDtypeStruct(tile_u.shape, f32)] + [jax.ShapeDtypeStruct((tiles, n, 2 * k), bf16)] * 2,
        cost_estimate=pl.CostEstimate(flops=6 * tiles * n * k * k * 2, bytes_accessed=20 * tiles * n * k, transcendentals=0),
        name="sketch_tiles",
    )(tile_u, tile_v, sketch)


def block_of(c, d, n):
    return lax.rem(c - d + n, n)


def project_kernel(n_col, at, mine, other, s_ref, full, small):
    r, c = at[0], at[1]
    chip, core = lax.shift_right_logical(r, 1), lax.rem(r, 2)
    chips, _, pair, piece, _ = mine.shape
    for src, parity in ((mine, core), (other, 1 - core)):
        for e in range(chips):
            for d in range(n_col):
                start = block_of(c, d, n_col) * (chips * piece) + (chip ^ e) * piece
                rows = pl.ds(pl.multiple_of(start, piece), piece)
                for t in range(pair):
                    full[parity * pair + t, rows, :] = beside(src[e, d, t])
    rhs = beside(s_ref[...])
    for j in range(full.shape[0]):
        x = fold(mm(full[j], rhs, TN))
        h = x.shape[0] // 2
        small[j] = x[:h] + x[h:]


def project(n_col, at, mine, other, sketch):
    chips, _, pair, piece, k = mine.shape
    tiles, n = 2 * pair, chips * n_col * piece
    vmem = pl.BlockSpec(memory_space=VMEM)
    return pl.pallas_call(
        functools.partial(project_kernel, n_col),
        in_specs=[pl.BlockSpec(memory_space=pltpu.SMEM)] + [vmem] * 3,
        out_specs=[vmem] * 2,
        out_shape=[jax.ShapeDtypeStruct((tiles, n, 2 * k), bf16), jax.ShapeDtypeStruct((tiles, k, k), f32)],
        cost_estimate=pl.CostEstimate(flops=6 * tiles * n * k * k, bytes_accessed=8 * tiles * n * k, transcendentals=0),
        name="project",
    )(at, mine, other, sketch)


def solve_kernel(n_col, at, diag, own_u, *refs):
    xs, outs = refs[:n_col], refs[n_col:]
    c = at[1]
    rows = diag.shape[0]
    solved = None
    for d in range(n_col):
        cols = pl.ds(pl.multiple_of(jnp.maximum(c - d, 0) * rows, rows), rows)
        x = xs[d][...] if d == 0 else jnp.where(c >= d, xs[d][...], 0.0)
        part = product(diag[:, cols], x)
        solved = part if solved is None else solved + part
    for d in range(n_col):
        cols = pl.ds(pl.multiple_of(jnp.maximum(c - d, 0) * rows, rows), rows)
        x = product_tn(solved, diag[:, cols]).T
        outs[d][...] = x if d == 0 else jnp.where(c >= d, x, own_u[...])


def solve(at, diag, own_u, xs):
    n_col = len(xs)
    rows, k = xs[0].shape
    vmem = pl.BlockSpec(memory_space=VMEM)
    return pl.pallas_call(
        functools.partial(solve_kernel, n_col),
        in_specs=[pl.BlockSpec(memory_space=pltpu.SMEM)] + [vmem] * (2 + n_col),
        out_specs=[vmem] * n_col,
        out_shape=[jax.ShapeDtypeStruct((rows, k), f32)] * n_col,
        compiler_params=pltpu.CompilerParams(vmem_limit_bytes=32 * 1024 * 1024),
        cost_estimate=pl.CostEstimate(flops=12 * n_col * rows * rows * k, bytes_accessed=4 * n_col * rows * rows, transcendentals=0),
        name="solve",
    )(at, diag, own_u, *xs)


def cores_kernel(n_col, at, *refs):
    parts, (mine, other), outs = refs[:n_col], refs[n_col : n_col + 2], refs[n_col + 2 :]
    r, c = at[0], at[1]
    chip, core = lax.shift_right_logical(r, 1), lax.rem(r, 2)
    total = parts[0][...]
    for d in range(1, n_col):
        total = total + jnp.where(c + d < n_col, parts[d][...], 0.0)
    lhs = beside(total.T)
    pair = mine.shape[1]
    for d in range(n_col):
        e = chip ^ lax.rem(c + d, n_col)
        for src, parity in ((mine, core), (other, 1 - core)):
            for t in range(pair):
                outs[d][parity * pair + t] = fold(mm(lhs, doubled_rows(src[e, t]), NN))


def partial_cores(at, parts, mine, other):
    n_col = len(parts)
    rows, k = parts[0].shape
    pair = mine.shape[1]
    vmem = pl.BlockSpec(memory_space=VMEM)
    return pl.pallas_call(
        functools.partial(cores_kernel, n_col),
        in_specs=[pl.BlockSpec(memory_space=pltpu.SMEM)] + [vmem] * (n_col + 2),
        out_specs=[vmem] * n_col,
        out_shape=[jax.ShapeDtypeStruct((2 * pair, k, k), f32)] * n_col,
        compiler_params=pltpu.CompilerParams(vmem_limit_bytes=32 * 1024 * 1024),
        cost_estimate=pl.CostEstimate(flops=12 * n_col * pair * rows * k * k, bytes_accessed=8 * n_col * pair * rows * k, transcendentals=0),
        name="partial_cores",
    )(at, *parts, mine, other)


def recompress_kernel(tiles, n, k, n_col, at, *refs):
    core_parts, first, second = refs[:n_col], refs[n_col : 2 * n_col], refs[2 * n_col : 3 * n_col]
    small, base, u_parts, v_parts, w_parts, new_u, new_v = refs[3 * n_col : 3 * n_col + 7]
    s, tu, tv, cu, sp, out, ru, work, cross, cores, row_parts, sem, row_sem = refs[3 * n_col + 7 :]
    c = at[1]
    root = math.sqrt(n)
    blk = n // n_col
    row_copies = []
    for d in range(n_col):
        rows = pl.ds(pl.multiple_of(block_of(c, d, n_col) * blk, blk), blk)
        row_copies.append(tuple(
            pltpu.make_async_copy(x, ru.at[rows], row_sem.at[d]) for x in (first[d], second[(n_col - d) % n_col])
        ))
    early, late, outs = [], [], []
    for t in range(tiles):
        early.append((
            pltpu.make_async_copy(base.at[t], s.at[t], sem.at[t]),
            pltpu.make_async_copy(u_parts.at[t], tu.at[t], sem.at[tiles + t]),
        ))
        late.append((
            pltpu.make_async_copy(v_parts.at[t], tv.at[t], sem.at[2 * tiles + t]),
            pltpu.make_async_copy(w_parts.at[t], cu.at[t], sem.at[3 * tiles + t]),
        ))
        outs.append((
            pltpu.make_async_copy(s.at[t], new_u.at[t], sem.at[4 * tiles + t]),
            pltpu.make_async_copy(out.at[t], new_v.at[t], sem.at[5 * tiles + t]),
        ))
    row_copies[0][0].start()
    for d in range(1, n_col):
        pl.when(c < d)(row_copies[d][0].start)
        pl.when(c >= d)(row_copies[d][1].start)
    for x in early[0] + early[1]:
        x.start()
    total = core_parts[0][...]
    for p in core_parts[1:]:
        total = total + p[...]
    cores[...] = total
    for x in row_copies:
        x[0].wait()

    def split(at):
        row_parts[at, :] = beside(ru[at, :])

    rows_loop(n, 512, split)
    for t in range(tiles):
        for x in early[t]:
            x.wait()
        for x in (early + late)[t + 2]:
            x.start()
        rhs = doubled_rows(-product(cores[t], small[t]))
        work[t] = jnp.zeros((k, 2 * k), f32)
        cross[t] = jnp.zeros((k, 2 * k), f32)

        def gather(at, t=t, rhs=rhs):
            part = beside(s[t, at, :] + fold(mm(row_parts[at, :], rhs, NN)))
            sp[t, at, :] = part
            x = mm(part, jnp.concatenate([part, tu[t, at, :], row_parts[at, :]], axis=1), TN)
            x = x[:k] + x[k:]
            work[t, :, :k] += fold(x[:, : 2 * k])
            cross[t, :, :k] += fold(x[:, 2 * k : 4 * k])
            cross[t, :, k:] += fold(x[:, 4 * k :])

        gather(pl.ds(0, n))
    for pair in late[2:]:
        for x in pair:
            x.start()
    eye = jnp.where(
        lax.broadcasted_iota(jnp.int32, (k, k), 0) == lax.broadcasted_iota(jnp.int32, (k, k), 1), 1.0, 0.0
    ).astype(f32)
    for t in range(tiles):
        work[t, :, k:] = eye
    eliminate(work, tiles, k)
    for t in range(tiles):
        inverse = work[t, :, k:]
        y = product(inverse, cross[t]) * (1.0 / root)
        c1 = y[:, :k]
        c2 = -product(y[:, k:], cores[t])
        by = doubled_columns(inverse * root)
        c12 = jnp.concatenate([doubled_columns(c1), doubled_columns(c2)], axis=1)
        for x in late[t]:
            x.wait()

        def finish(at, t=t, by=by, c12=c12):
            s[t, at, :] = fold(mm(sp[t, at, :], by, NT))
            lhs = jnp.concatenate([tv[t, at, :], cu[t, at, :]], axis=1)
            out[t, at, :] = fold(mm(lhs, c12, NT))

        finish(pl.ds(0, n))
        for x in outs[t]:
            x.start()
    for pair in outs:
        for x in pair:
            x.wait()


def recompress(at, core_parts, first, second, small, base, u_parts, v_parts, w_parts):
    tiles, n, k = base.shape
    n_col = len(core_parts)
    any_ = pl.BlockSpec(memory_space=ANY)
    vmem = pl.BlockSpec(memory_space=VMEM)
    full = lambda: VMEM((tiles, n, k), f32)
    split = lambda: VMEM((tiles, n, 2 * k), bf16)
    return pl.pallas_call(
        functools.partial(recompress_kernel, tiles, n, k, n_col),
        in_specs=[pl.BlockSpec(memory_space=pltpu.SMEM)] + [vmem] * n_col + [any_] * (2 * n_col) + [vmem] + [any_] * 4,
        out_specs=[any_, any_],
        out_shape=[jax.ShapeDtypeStruct(base.shape, f32)] * 2,
        scratch_shapes=[
            full(), split(), split(), split(), split(), full(), VMEM((n, k), f32),
            VMEM((tiles, k, 2 * k), f32), VMEM((tiles, k, 2 * k), f32), VMEM((tiles, k, k), f32),
            VMEM((n, 2 * k), bf16),
            pltpu.SemaphoreType.DMA((6 * tiles,)), pltpu.SemaphoreType.DMA((n_col,)),
        ],
        cost_estimate=pl.CostEstimate(flops=24 * tiles * n * k * k, bytes_accessed=28 * tiles * n * k, transcendentals=0),
        name="recompress",
    )(at, *core_parts, *first, *second, small, base, u_parts, v_parts, w_parts)


def step(n_row, n_col, tile_u, tile_v, row_panel_u, row_panel_v, col_panel_u, col_panel_v, diag_inverse, sketch):
    chips = n_row // 2
    r, c = lax.axis_index("row"), lax.axis_index("col")
    at = jnp.stack([r, c]).astype(jnp.int32)
    chip = lax.shift_right_logical(r, 1)

    def partner(x, m):
        return lax.ppermute(x, "row", [(a, a ^ m) for a in range(n_row)])

    def shift(x, pairs):
        return lax.ppermute(x, "col", pairs)

    def around(x, d):
        return shift(x, [(a, (a + d) % n_col) for a in range(n_col)])

    def pick(x, i, axis=0):
        return lax.dynamic_index_in_dim(x, i, axis, keepdims=False)

    row_v, row_u = row_panel_v[0], row_panel_u[0]
    loads = [jnp.where(c + d < n_col, row_v, row_u) for d in range(1, n_col)]
    first = [around(x, d) for d, x in enumerate(loads, 1)]
    col_v_mine = jnp.stack([col_panel_v] + [partner(col_panel_v, 2 * e) for e in range(1, chips)])
    pair, rows, k = col_panel_u.shape
    cut = col_panel_u.reshape(pair, chips, rows // chips, k)
    cuts = jnp.stack([pick(cut, chip, 1)] + [partner(pick(cut, chip ^ e, 1), 2 * e) for e in range(1, chips)])
    col_v_other = partner(col_v_mine, 1)
    moved = [pick(cuts, chip ^ c)] + [around(pick(cuts, chip ^ lax.rem(c + d, n_col)), d) for d in range(1, n_col)]
    planes = lax.optimization_barrier(jnp.stack(moved))
    base, u_parts, v_parts = sketch_tiles(tile_u[0], tile_v[0], sketch)
    sums = solve(at, diag_inverse, row_u, [row_v] + first)
    second = [around(sums[d], n_col - d) for d in range(1, n_col)]
    gathered = [planes] + [partner(planes, 2 * e) for e in range(1, chips)]
    col_u_mine = jnp.stack(gathered)
    col_u_other = partner(col_u_mine, 1)
    w_parts, small = project(n_col, at, col_u_mine, col_u_other, sketch)
    cores = partial_cores(at, [sums[0]] + second, col_v_mine, col_v_other)
    core_parts = [cores[0]] + [around(cores[d], d) for d in range(1, n_col)]
    new_u, new_v = recompress(at, core_parts, [row_u] + first, [row_u] + second, small, base, u_parts, v_parts, w_parts)
    return new_u[None], new_v[None]


def solution(mesh):
    n_row, n_col = mesh.shape["row"], mesh.shape["col"]
    in_specs = (
        P("row", "col", None, None),
        P("row", "col", None, None),
        P("row", "col", None),
        P("row", "col", None),
        P("row", "col", None),
        P("row", "col", None),
        P("col", None),
        P(),
    )
    out_specs = (P("row", "col", None, None), P("row", "col", None, None))

    def body(*args):
        return step(n_row, n_col, *args)

    return jax.shard_map(body, mesh=mesh, in_specs=in_specs, out_specs=out_specs, check_vma=False)
```

```python
import functools
import math

import jax
import jax.numpy as jnp
from jax import lax
from jax.experimental import pallas as pl
from jax.experimental.pallas import tpu as pltpu
from jax.sharding import PartitionSpec as P

f32, bf16 = jnp.float32, jnp.bfloat16
ANY, VMEM = pl.ANY, pltpu.VMEM
NT = (((1,), (1,)), ((), ()))
NN = (((1,), (0,)), ((), ()))
TN = (((0,), (0,)), ((), ()))


def mm(a, b, dims):
    return lax.dot_general(a, b, dims, preferred_element_type=f32)


def halves(x):
    hi = x.astype(bf16)
    return hi, (x - hi.astype(f32)).astype(bf16)


def beside(x):
    return jnp.concatenate(halves(x), axis=1)


def doubled_rows(x):
    both = beside(x)
    return jnp.concatenate([both, both], axis=0)


def doubled_columns(x):
    hi, lo = halves(x)
    return jnp.concatenate([jnp.concatenate([hi, hi], axis=1), jnp.concatenate([lo, lo], axis=1)], axis=0)


def fold(x):
    w = x.shape[1] // 2
    return x[:, :w] + x[:, w:]


def product(a, b):
    return fold(mm(beside(a), doubled_rows(b), NN))


def product_tn(a, b):
    x = fold(mm(beside(a), beside(b), TN))
    h = x.shape[0] // 2
    return x[:h] + x[h:]


def thirds(x):
    a = x.astype(bf16).astype(f32)
    r = x - a
    b = r.astype(bf16).astype(f32)
    return a, b, r - b


def eliminate(work, tiles, k):
    b = 8
    row = lax.broadcasted_iota(jnp.int32, (b, k), 0)
    for top in range(0, k, b):
        left, right, cols, scale = [], [], [], []
        for t in range(tiles):
            x = work[t, top : top + b, :]
            left.append(x[:, :k])
            right.append(x[:, k:])
            cols.append([jnp.broadcast_to(x[:, top + j : top + j + 1], (b, k)) for j in range(b)])
            scale.append(jnp.zeros((b, k), f32))
        for j in range(b):
            for t in range(tiles):
                pivot = jnp.broadcast_to(cols[t][j][j : j + 1, :], (b, k))
                inverse = 1.0 / pivot
                scale[t] = jnp.where(row == j, inverse, scale[t])
                if j + 1 < b:
                    m = jnp.where(row > j, cols[t][j] * inverse, 0.0)
                    for u in range(j + 1, b):
                        cols[t][u] = cols[t][u] - m * cols[t][u][j : j + 1, :]
                    left[t] = left[t] - m * left[t][j : j + 1, :]
                    right[t] = right[t] - m * right[t][j : j + 1, :]
        for t in range(tiles):
            work[t, top : top + b, k:] = right[t] * jnp.sqrt(scale[t])
        if top + b < k:
            for t in range(tiles):
                p0, p1, p2 = thirds(left[t] * scale[t])
                q0, q1, q2 = thirds(jnp.concatenate([left[t], right[t]], axis=1))
                p = jnp.concatenate([p0, p1, p0, p2, p0, p1], axis=0).astype(bf16)
                q = jnp.concatenate([q0, q0, q1, q0, q2, q1], axis=0).astype(bf16)
                update = mm(p, q, TN)
                work[t, top + b :, :] = work[t, top + b :, :] - update[top + b :, :]


def quadrants(x):
    x = fold(x)
    h = x.shape[0] // 2
    return x[:h] + x[h:]


def sketched(u_ref, v_ref, s_ref, out_ref, v_parts, u_parts, cross):
    v = beside(v_ref[0])
    v_parts[0] = v
    rhs = doubled_rows(quadrants(mm(v, beside(s_ref[...]), TN)))
    u = beside(u_ref[0])
    u_parts[0] = u
    x = fold(mm(u, rhs, NN))
    out_ref[0] = x
    cross[0] = quadrants(mm(beside(x), u, TN))


def sketch_tiles(tile_u, tile_v, sketch, begin, end):
    _, n, k = tile_u.shape
    tiles = end - begin
    block = pl.BlockSpec((1, n, k), lambda i: (i + begin, 0, 0))
    own = lambda *dims: pl.BlockSpec((1, *dims), lambda i: (i, 0, 0))
    return pl.pallas_call(
        sketched,
        grid=(tiles,),
        in_specs=[block, block, pl.BlockSpec((n, k), lambda i: (0, 0))],
        out_specs=[own(n, k), own(n, 2 * k), own(n, 2 * k), own(k, k)],
        out_shape=[jax.ShapeDtypeStruct((tiles, n, k), f32)]
        + [jax.ShapeDtypeStruct((tiles, n, 2 * k), bf16)] * 2
        + [jax.ShapeDtypeStruct((tiles, k, k), f32)],
        compiler_params=pltpu.CompilerParams(vmem_limit_bytes=36 * 1024 * 1024),
        cost_estimate=pl.CostEstimate(flops=6 * tiles * n * k * k * 2, bytes_accessed=20 * tiles * n * k, transcendentals=0),
        name="sketch_tiles",
    )(tile_u, tile_v, sketch)


def split_kernel(diag, parts):
    rows = diag.shape[0]
    for b in range(parts.shape[0]):
        parts[b] = beside(diag[:, b * rows : (b + 1) * rows])


def split_diag(diag):
    rows, n = diag.shape
    vmem = pl.BlockSpec(memory_space=VMEM)
    return pl.pallas_call(
        split_kernel,
        in_specs=[vmem],
        out_specs=vmem,
        out_shape=jax.ShapeDtypeStruct((n // rows, rows, 2 * rows), bf16),
        compiler_params=pltpu.CompilerParams(vmem_limit_bytes=36 * 1024 * 1024),
        cost_estimate=pl.CostEstimate(flops=4 * rows * n, bytes_accessed=8 * rows * n, transcendentals=0),
        name="split_diag",
    )(diag)


def block_of(c, d, n):
    return lax.rem(c - d + n, n)


def project_kernel(n_col, at, mine, other, s_ref, full, small):
    r, c = at[0], at[1]
    chip, core = lax.shift_right_logical(r, 1), lax.rem(r, 2)
    chips, _, pair, piece, _ = mine.shape
    for src, parity in ((mine, core), (other, 1 - core)):
        for e in range(chips):
            for d in range(n_col):
                start = block_of(c, d, n_col) * (chips * piece) + (chip ^ e) * piece
                rows = pl.ds(pl.multiple_of(start, piece), piece)
                for t in range(pair):
                    full[parity * pair + t, rows, :] = beside(src[e, d, t])
    rhs = beside(s_ref[...])
    for j in range(full.shape[0]):
        x = fold(mm(full[j], rhs, TN))
        h = x.shape[0] // 2
        small[j] = x[:h] + x[h:]


def project(n_col, at, mine, other, sketch):
    chips, _, pair, piece, k = mine.shape
    tiles, n = 2 * pair, chips * n_col * piece
    vmem = pl.BlockSpec(memory_space=VMEM)
    return pl.pallas_call(
        functools.partial(project_kernel, n_col),
        in_specs=[pl.BlockSpec(memory_space=pltpu.SMEM)] + [vmem] * 3,
        out_specs=[vmem] * 2,
        out_shape=[jax.ShapeDtypeStruct((tiles, n, 2 * k), bf16), jax.ShapeDtypeStruct((tiles, k, k), f32)],
        compiler_params=pltpu.CompilerParams(vmem_limit_bytes=36 * 1024 * 1024),
        cost_estimate=pl.CostEstimate(flops=6 * tiles * n * k * k, bytes_accessed=8 * tiles * n * k, transcendentals=0),
        name="project",
    )(at, mine, other, sketch)


def solve_kernel(n_col, at, diag, own_u, *refs):
    xs, outs = refs[:n_col], refs[n_col:]
    c = at[1]
    solved = None
    for d in range(n_col):
        x = xs[d][...] if d == 0 else jnp.where(c >= d, xs[d][...], 0.0)
        part = fold(mm(diag[jnp.maximum(c - d, 0)], doubled_rows(x), NN))
        solved = part if solved is None else solved + part
    lhs = beside(solved)
    for d in range(n_col):
        x = quadrants(mm(lhs, diag[jnp.maximum(c - d, 0)], TN)).T
        outs[d][...] = x if d == 0 else jnp.where(c >= d, x, own_u[...])


def solve(at, diag, own_u, xs):
    n_col = len(xs)
    rows, k = xs[0].shape
    vmem = pl.BlockSpec(memory_space=VMEM)
    return pl.pallas_call(
        functools.partial(solve_kernel, n_col),
        in_specs=[pl.BlockSpec(memory_space=pltpu.SMEM)] + [vmem] * (2 + n_col),
        out_specs=[vmem] * n_col,
        out_shape=[jax.ShapeDtypeStruct((rows, k), f32)] * n_col,
        compiler_params=pltpu.CompilerParams(vmem_limit_bytes=32 * 1024 * 1024),
        cost_estimate=pl.CostEstimate(flops=12 * n_col * rows * rows * k, bytes_accessed=4 * n_col * rows * rows, transcendentals=0),
        name="solve",
    )(at, diag, own_u, *xs)


def cores_kernel(n_col, at, *refs):
    parts, (mine, other), outs = refs[:n_col], refs[n_col : n_col + 2], refs[n_col + 2 :]
    r, c = at[0], at[1]
    chip, core = lax.shift_right_logical(r, 1), lax.rem(r, 2)
    total = parts[0][...]
    for d in range(1, n_col):
        total = total + jnp.where(c + d < n_col, parts[d][...], 0.0)
    lhs = beside(total.T)
    pair = mine.shape[1]
    for d in range(n_col):
        e = chip ^ lax.rem(c + d, n_col)
        for src, parity in ((mine, core), (other, 1 - core)):
            for t in range(pair):
                outs[d][parity * pair + t] = fold(mm(lhs, doubled_rows(src[e, t]), NN))


def partial_cores(at, parts, mine, other):
    n_col = len(parts)
    rows, k = parts[0].shape
    pair = mine.shape[1]
    vmem = pl.BlockSpec(memory_space=VMEM)
    return pl.pallas_call(
        functools.partial(cores_kernel, n_col),
        in_specs=[pl.BlockSpec(memory_space=pltpu.SMEM)] + [vmem] * (n_col + 2),
        out_specs=[vmem] * n_col,
        out_shape=[jax.ShapeDtypeStruct((2 * pair, k, k), f32)] * n_col,
        compiler_params=pltpu.CompilerParams(vmem_limit_bytes=32 * 1024 * 1024),
        cost_estimate=pl.CostEstimate(flops=12 * n_col * pair * rows * k * k, bytes_accessed=8 * n_col * pair * rows * k, transcendentals=0),
        name="partial_cores",
    )(at, *parts, mine, other)


def prepare_kernel(n_col, at, *refs):
    first, second = refs[:n_col], refs[n_col : 2 * n_col]
    halves_in, (row_parts, with_row, row_row) = refs[2 * n_col : -3], refs[-3:]
    c = at[1]
    blk = first[0].shape[0]
    for d in range(n_col):
        rows = pl.ds(pl.multiple_of(block_of(c, d, n_col) * blk, blk), blk)
        x = first[0][...] if d == 0 else jnp.where(c < d, first[d][...], second[n_col - d][...])
        row_parts[rows, :] = beside(x)
    row = row_parts[...]
    row_row[...] = quadrants(mm(row, row, TN))
    t = 0
    for i in range(0, len(halves_in), 2):
        base, u_parts = halves_in[i : i + 2]
        for j in range(base.shape[0]):
            x = mm(row, jnp.concatenate([beside(base[j]), u_parts[j]], axis=1), TN)
            k = x.shape[0] // 2
            with_row[t] = jnp.concatenate([quadrants(x[:, : 2 * k]), quadrants(x[:, 2 * k :])], axis=1)
            t += 1


def prepare(at, first, second, groups):
    n_col = len(first)
    blk, k = first[0].shape
    n = n_col * blk
    tiles = sum(base.shape[0] for base, _ in groups)
    vmem = pl.BlockSpec(memory_space=VMEM)
    return pl.pallas_call(
        functools.partial(prepare_kernel, n_col),
        in_specs=[pl.BlockSpec(memory_space=pltpu.SMEM)] + [vmem] * (2 * n_col + 2 * len(groups)),
        out_specs=[vmem] * 3,
        out_shape=[
            jax.ShapeDtypeStruct((n, 2 * k), bf16),
            jax.ShapeDtypeStruct((tiles, k, 2 * k), f32),
            jax.ShapeDtypeStruct((k, k), f32),
        ],
        compiler_params=pltpu.CompilerParams(vmem_limit_bytes=36 * 1024 * 1024),
        cost_estimate=pl.CostEstimate(flops=12 * tiles * n * k * k, bytes_accessed=8 * tiles * n * k, transcendentals=0),
        name="prepare",
    )(at, *first, *second, *[x for pair in groups for x in pair])


def recompress_kernel(n, k, n_col, sizes, *refs):
    tiles = sum(sizes)
    place = [(g, j) for g, size in enumerate(sizes) for j in range(size)]
    groups = len(sizes)
    core_parts, refs = refs[:n_col], refs[n_col:]
    (small, with_row, row_row), refs = refs[:3], refs[3:]
    crosses, refs = refs[:groups], refs[groups:]
    bases, v_parts, refs = refs[:groups], refs[groups : 2 * groups], refs[2 * groups :]
    (w_parts, row_in, new_u, new_v), refs = refs[:4], refs[4:]
    s, tv, cu, sp, out, work, cross, cores, row_parts, sem, row_sem = refs
    root = math.sqrt(n)
    row_copy = pltpu.make_async_copy(row_in, row_parts, row_sem)
    early, late, outs = [], [], []
    for t, (g, j) in enumerate(place):
        early.append(pltpu.make_async_copy(bases[g].at[j], s.at[t], sem.at[t]))
        late.append((
            pltpu.make_async_copy(v_parts[g].at[j], tv.at[t], sem.at[tiles + t]),
            pltpu.make_async_copy(w_parts.at[t], cu.at[t], sem.at[2 * tiles + t]),
        ))
        outs.append((
            pltpu.make_async_copy(s.at[t], new_u.at[t], sem.at[3 * tiles + t]),
            pltpu.make_async_copy(out.at[t], new_v.at[t], sem.at[4 * tiles + t]),
        ))
    row_copy.start()
    for x in early:
        x.start()
    total = core_parts[0][...]
    for p in core_parts[1:]:
        total = total + p[...]
    cores[...] = total
    eye = jnp.where(
        lax.broadcasted_iota(jnp.int32, (k, k), 0) == lax.broadcasted_iota(jnp.int32, (k, k), 1), 1.0, 0.0
    ).astype(f32)
    mixes = [-product(cores[t], small[t]) for t in range(tiles)]
    row_copy.wait()
    for t, (g, j) in enumerate(place):
        early[t].wait()
        part = beside(s[t] + fold(mm(row_parts[...], doubled_rows(mixes[t]), NN)))
        sp[t] = part
        work[t, :, :k] = quadrants(mm(part, part, TN))
        work[t, :, k:] = eye
        x = product_tn(mixes[t], jnp.concatenate([with_row[t, :, k:], row_row[...]], axis=1))
        cross[t] = x + jnp.concatenate([crosses[g][j], with_row[t, :, :k].T], axis=1)
        for x in late[t]:
            x.start()
    eliminate(work, tiles, k)
    for t in range(tiles):
        inverse = work[t, :, k:]
        y = product(inverse, cross[t]) * (1.0 / root)
        c1 = y[:, :k]
        c2 = -product(y[:, k:], cores[t])
        by = doubled_columns(inverse * root)
        c12 = jnp.concatenate([doubled_columns(c1), doubled_columns(c2)], axis=1)
        for x in late[t]:
            x.wait()
        s[t] = fold(mm(sp[t], by, NT))
        outs[t][0].start()
        out[t] = fold(mm(jnp.concatenate([tv[t], cu[t]], axis=1), c12, NT))
        outs[t][1].start()
    for pair in outs:
        for x in pair:
            x.wait()


def recompress(core_parts, small, with_row, row_row, crosses, bases, v_parts, w_parts, row_parts):
    tiles, n, k2 = w_parts.shape
    k = k2 // 2
    n_col = len(core_parts)
    sizes = [x.shape[0] for x in bases]
    groups = len(sizes)
    any_ = pl.BlockSpec(memory_space=ANY)
    vmem = pl.BlockSpec(memory_space=VMEM)
    full = lambda: VMEM((tiles, n, k), f32)
    split = lambda: VMEM((tiles, n, 2 * k), bf16)
    return pl.pallas_call(
        functools.partial(recompress_kernel, n, k, n_col, sizes),
        in_specs=[vmem] * (n_col + 3 + groups) + [any_] * (2 * groups + 2),
        out_specs=[any_, any_],
        out_shape=[jax.ShapeDtypeStruct((tiles, n, k), f32)] * 2,
        scratch_shapes=[
            full(), split(), split(), split(), full(),
            VMEM((tiles, k, 2 * k), f32), VMEM((tiles, k, 2 * k), f32), VMEM((tiles, k, k), f32),
            VMEM((n, 2 * k), bf16),
            pltpu.SemaphoreType.DMA((5 * tiles,)), pltpu.SemaphoreType.DMA,
        ],
        cost_estimate=pl.CostEstimate(flops=24 * tiles * n * k * k, bytes_accessed=28 * tiles * n * k, transcendentals=0),
        name="recompress",
    )(*core_parts, small, with_row, row_row, *crosses, *bases, *v_parts, w_parts, row_parts)


def step(n_row, n_col, tile_u, tile_v, row_panel_u, row_panel_v, col_panel_u, col_panel_v, diag_inverse, sketch):
    chips = n_row // 2
    r, c = lax.axis_index("row"), lax.axis_index("col")
    at = jnp.stack([r, c]).astype(jnp.int32)
    chip = lax.shift_right_logical(r, 1)

    def partner(x, m):
        return lax.ppermute(x, "row", [(a, a ^ m) for a in range(n_row)])

    def shift(x, pairs):
        return lax.ppermute(x, "col", pairs)

    def around(x, d):
        return shift(x, [(a, (a + d) % n_col) for a in range(n_col)])

    def pick(x, i, axis=0):
        return lax.dynamic_index_in_dim(x, i, axis, keepdims=False)

    row_v, row_u = row_panel_v[0], row_panel_u[0]
    loads = [jnp.where(c + d < n_col, row_v, row_u) for d in range(1, n_col)]
    first = [around(x, d) for d, x in enumerate(loads, 1)]
    col_v_mine = jnp.stack([col_panel_v] + [partner(col_panel_v, 2 * e) for e in range(1, chips)])
    pair, rows, k = col_panel_u.shape
    cut = col_panel_u.reshape(pair, chips, rows // chips, k)
    cuts = jnp.stack([pick(cut, chip, 1)] + [partner(pick(cut, chip ^ e, 1), 2 * e) for e in range(1, chips)])
    col_v_other = partner(col_v_mine, 1)
    moved = [pick(cuts, chip ^ c)] + [around(pick(cuts, chip ^ lax.rem(c + d, n_col)), d) for d in range(1, n_col)]
    planes = lax.optimization_barrier(jnp.stack(moved))
    tiles = tile_u.shape[1]
    diag = split_diag(diag_inverse)
    groups = []
    for begin, end in ((0, tiles // 2), (tiles // 2, tiles)):
        groups.append(sketch_tiles(tile_u[0], tile_v[0], sketch, begin, end))
    bases, v_parts, u_parts, crosses = zip(*groups)
    sums = solve(at, diag, row_u, [row_v] + first)
    second = [around(sums[d], n_col - d) for d in range(1, n_col)]
    gathered = [planes] + [partner(planes, 2 * e) for e in range(1, chips)]
    col_u_mine = jnp.stack(gathered)
    col_u_other = partner(col_u_mine, 1)
    w_parts, small = project(n_col, at, col_u_mine, col_u_other, sketch)
    cores = partial_cores(at, [sums[0]] + second, col_v_mine, col_v_other)
    core_parts = [cores[0]] + [around(cores[d], d) for d in range(1, n_col)]
    row_parts, with_row, row_row = prepare(at, [row_u] + first, [row_u] + second, list(zip(bases, u_parts)))
    new_u, new_v = recompress(core_parts, small, with_row, row_row, crosses, bases, v_parts, w_parts, row_parts)
    return new_u[None], new_v[None]


def solution(mesh):
    n_row, n_col = mesh.shape["row"], mesh.shape["col"]
    in_specs = (
        P("row", "col", None, None),
        P("row", "col", None, None),
        P("row", "col", None),
        P("row", "col", None),
        P("row", "col", None),
        P("row", "col", None),
        P("col", None),
        P(),
    )
    out_specs = (P("row", "col", None, None), P("row", "col", None, None))

    def body(*args):
        return step(n_row, n_col, *args)

    return jax.shard_map(body, mesh=mesh, in_specs=in_specs, out_specs=out_specs, check_vma=False)
```

```python
import functools
import math

import jax
import jax.numpy as jnp
from jax import lax
from jax.experimental import pallas as pl
from jax.experimental.pallas import tpu as pltpu
from jax.sharding import PartitionSpec as P

f32, bf16 = jnp.float32, jnp.bfloat16
ANY, VMEM = pl.ANY, pltpu.VMEM
NT = (((1,), (1,)), ((), ()))
NN = (((1,), (0,)), ((), ()))
TN = (((0,), (0,)), ((), ()))


def mm(a, b, dims):
    return lax.dot_general(a, b, dims, preferred_element_type=f32)


def halves(x):
    hi = x.astype(bf16)
    return hi, (x - hi.astype(f32)).astype(bf16)


def beside(x):
    return jnp.concatenate(halves(x), axis=1)


def doubled_rows(x):
    both = beside(x)
    return jnp.concatenate([both, both], axis=0)


def doubled_columns(x):
    hi, lo = halves(x)
    return jnp.concatenate([jnp.concatenate([hi, hi], axis=1), jnp.concatenate([lo, lo], axis=1)], axis=0)


def fold(x):
    w = x.shape[1] // 2
    return x[:, :w] + x[:, w:]


def product(a, b):
    return fold(mm(beside(a), doubled_rows(b), NN))


def product_tn(a, b):
    x = fold(mm(beside(a), beside(b), TN))
    h = x.shape[0] // 2
    return x[:h] + x[h:]


def thirds(x):
    a = x.astype(bf16).astype(f32)
    r = x - a
    b = r.astype(bf16).astype(f32)
    return a, b, r - b


def eliminate(work, tiles, k):
    b = 16 if k % 16 == 0 else 8
    row = lax.broadcasted_iota(jnp.int32, (b, k), 0)
    for top in range(0, k, b):
        left, right, cols, scale = [], [], [], []
        for t in range(tiles):
            x = work[t, top : top + b, :]
            left.append(x[:, :k])
            right.append(x[:, k:])
            cols.append([jnp.broadcast_to(x[:, top + j : top + j + 1], (b, k)) for j in range(b)])
            scale.append(jnp.zeros((b, k), f32))
        for j in range(b):
            for t in range(tiles):
                pivot = jnp.broadcast_to(cols[t][j][j : j + 1, :], (b, k))
                inverse = 1.0 / pivot
                scale[t] = jnp.where(row == j, inverse, scale[t])
                if j + 1 < b:
                    m = jnp.where(row > j, cols[t][j] * inverse, 0.0)
                    for u in range(j + 1, b):
                        cols[t][u] = cols[t][u] - m * cols[t][u][j : j + 1, :]
                    left[t] = left[t] - m * left[t][j : j + 1, :]
                    right[t] = right[t] - m * right[t][j : j + 1, :]
        for t in range(tiles):
            work[t, top : top + b, k:] = right[t] * jnp.sqrt(scale[t])
        if top + b < k:
            for t in range(tiles):
                p0, p1, p2 = thirds(left[t] * scale[t])
                q0, q1, q2 = thirds(jnp.concatenate([left[t], right[t]], axis=1))
                p = jnp.concatenate([p0, p1, p0, p2, p0, p1], axis=0).astype(bf16)
                q = jnp.concatenate([q0, q0, q1, q0, q2, q1], axis=0).astype(bf16)
                update = mm(p, q, TN)
                work[t, top + b :, :] = work[t, top + b :, :] - update[top + b :, :]


def quadrants(x):
    x = fold(x)
    h = x.shape[0] // 2
    return x[:h] + x[h:]


def sketched(u_ref, v_ref, s_ref, out_ref, v_parts, u_parts, cross):
    v = beside(v_ref[0])
    v_parts[0] = v
    rhs = doubled_rows(quadrants(mm(v, beside(s_ref[...]), TN)))
    u = beside(u_ref[0])
    u_parts[0] = u
    x = fold(mm(u, rhs, NN))
    out_ref[0] = x
    cross[0] = quadrants(mm(beside(x), u, TN))


def sketch_tiles(tile_u, tile_v, sketch, begin, end):
    _, n, k = tile_u.shape
    tiles = end - begin
    block = pl.BlockSpec((1, n, k), lambda i: (i + begin, 0, 0))
    own = lambda *dims: pl.BlockSpec((1, *dims), lambda i: (i, 0, 0))
    return pl.pallas_call(
        sketched,
        grid=(tiles,),
        in_specs=[block, block, pl.BlockSpec((n, k), lambda i: (0, 0))],
        out_specs=[own(n, k), own(n, 2 * k), own(n, 2 * k), own(k, k)],
        out_shape=[jax.ShapeDtypeStruct((tiles, n, k), f32)]
        + [jax.ShapeDtypeStruct((tiles, n, 2 * k), bf16)] * 2
        + [jax.ShapeDtypeStruct((tiles, k, k), f32)],
        compiler_params=pltpu.CompilerParams(vmem_limit_bytes=57 * 1024 * 1024),
        cost_estimate=pl.CostEstimate(flops=6 * tiles * n * k * k * 2, bytes_accessed=20 * tiles * n * k, transcendentals=0),
        name="sketch_tiles",
    )(tile_u, tile_v, sketch)


def split_kernel(diag, parts):
    rows = diag.shape[0]
    for b in range(parts.shape[0]):
        parts[b] = beside(diag[:, b * rows : (b + 1) * rows])


def split_diag(diag):
    rows, n = diag.shape
    vmem = pl.BlockSpec(memory_space=VMEM)
    return pl.pallas_call(
        split_kernel,
        in_specs=[vmem],
        out_specs=vmem,
        out_shape=jax.ShapeDtypeStruct((n // rows, rows, 2 * rows), bf16),
        compiler_params=pltpu.CompilerParams(vmem_limit_bytes=36 * 1024 * 1024),
        cost_estimate=pl.CostEstimate(flops=4 * rows * n, bytes_accessed=8 * rows * n, transcendentals=0),
        name="split_diag",
    )(diag)


def block_of(c, d, n):
    return lax.rem(c - d + n, n)


def project_kernel(n_col, at, mine, other, s_ref, full, small):
    r, c = at[0], at[1]
    chip, core = lax.shift_right_logical(r, 1), lax.rem(r, 2)
    chips, _, pair, piece, _ = mine.shape
    for src, parity in ((mine, core), (other, 1 - core)):
        for e in range(chips):
            for d in range(n_col):
                start = block_of(c, d, n_col) * (chips * piece) + (chip ^ e) * piece
                rows = pl.ds(pl.multiple_of(start, piece), piece)
                for t in range(pair):
                    full[parity * pair + t, rows, :] = beside(src[e, d, t])
    rhs = beside(s_ref[...])
    for j in range(full.shape[0]):
        x = fold(mm(full[j], rhs, TN))
        h = x.shape[0] // 2
        small[j] = x[:h] + x[h:]


def project(n_col, at, mine, other, sketch):
    chips, _, pair, piece, k = mine.shape
    tiles, n = 2 * pair, chips * n_col * piece
    vmem = pl.BlockSpec(memory_space=VMEM)
    return pl.pallas_call(
        functools.partial(project_kernel, n_col),
        in_specs=[pl.BlockSpec(memory_space=pltpu.SMEM)] + [vmem] * 3,
        out_specs=[vmem] * 2,
        out_shape=[jax.ShapeDtypeStruct((tiles, n, 2 * k), bf16), jax.ShapeDtypeStruct((tiles, k, k), f32)],
        compiler_params=pltpu.CompilerParams(vmem_limit_bytes=36 * 1024 * 1024),
        cost_estimate=pl.CostEstimate(flops=6 * tiles * n * k * k, bytes_accessed=8 * tiles * n * k, transcendentals=0),
        name="project",
    )(at, mine, other, sketch)


def solve_kernel(n_col, at, diag, own_u, *refs):
    xs, outs = refs[:n_col], refs[n_col:]
    c = at[1]
    solved = None
    for d in range(n_col):
        x = xs[d][...] if d == 0 else jnp.where(c >= d, xs[d][...], 0.0)
        part = fold(mm(diag[jnp.maximum(c - d, 0)], doubled_rows(x), NN))
        solved = part if solved is None else solved + part
    lhs = beside(solved)
    for d in range(n_col):
        x = quadrants(mm(lhs, diag[jnp.maximum(c - d, 0)], TN)).T
        outs[d][...] = x if d == 0 else jnp.where(c >= d, x, own_u[...])


def solve(at, diag, own_u, xs):
    n_col = len(xs)
    rows, k = xs[0].shape
    vmem = pl.BlockSpec(memory_space=VMEM)
    return pl.pallas_call(
        functools.partial(solve_kernel, n_col),
        in_specs=[pl.BlockSpec(memory_space=pltpu.SMEM)] + [vmem] * (2 + n_col),
        out_specs=[vmem] * n_col,
        out_shape=[jax.ShapeDtypeStruct((rows, k), f32)] * n_col,
        compiler_params=pltpu.CompilerParams(vmem_limit_bytes=32 * 1024 * 1024),
        cost_estimate=pl.CostEstimate(flops=12 * n_col * rows * rows * k, bytes_accessed=4 * n_col * rows * rows, transcendentals=0),
        name="solve",
    )(at, diag, own_u, *xs)


def cores_kernel(n_col, at, *refs):
    parts, (mine, other), outs = refs[:n_col], refs[n_col : n_col + 2], refs[n_col + 2 :]
    r, c = at[0], at[1]
    chip, core = lax.shift_right_logical(r, 1), lax.rem(r, 2)
    total = parts[0][...]
    for d in range(1, n_col):
        total = total + jnp.where(c + d < n_col, parts[d][...], 0.0)
    lhs = beside(total.T)
    pair = mine.shape[1]
    for d in range(n_col):
        e = chip ^ lax.rem(c + d, n_col)
        for src, parity in ((mine, core), (other, 1 - core)):
            for t in range(pair):
                outs[d][parity * pair + t] = fold(mm(lhs, doubled_rows(src[e, t]), NN))


def partial_cores(at, parts, mine, other):
    n_col = len(parts)
    rows, k = parts[0].shape
    pair = mine.shape[1]
    vmem = pl.BlockSpec(memory_space=VMEM)
    return pl.pallas_call(
        functools.partial(cores_kernel, n_col),
        in_specs=[pl.BlockSpec(memory_space=pltpu.SMEM)] + [vmem] * (n_col + 2),
        out_specs=[vmem] * n_col,
        out_shape=[jax.ShapeDtypeStruct((2 * pair, k, k), f32)] * n_col,
        compiler_params=pltpu.CompilerParams(vmem_limit_bytes=32 * 1024 * 1024),
        cost_estimate=pl.CostEstimate(flops=12 * n_col * pair * rows * k * k, bytes_accessed=8 * n_col * pair * rows * k, transcendentals=0),
        name="partial_cores",
    )(at, *parts, mine, other)


def prepare_kernel(n_col, at, *refs):
    first, second = refs[:n_col], refs[n_col : 2 * n_col]
    halves_in, (row_parts, with_row, row_row) = refs[2 * n_col : -3], refs[-3:]
    c = at[1]
    blk = first[0].shape[0]
    for d in range(n_col):
        rows = pl.ds(pl.multiple_of(block_of(c, d, n_col) * blk, blk), blk)
        x = first[0][...] if d == 0 else jnp.where(c < d, first[d][...], second[n_col - d][...])
        row_parts[rows, :] = beside(x)
    row = row_parts[...]
    row_row[...] = quadrants(mm(row, row, TN))
    t = 0
    for i in range(0, len(halves_in), 2):
        base, u_parts = halves_in[i : i + 2]
        for j in range(base.shape[0]):
            x = mm(row, jnp.concatenate([beside(base[j]), u_parts[j]], axis=1), TN)
            k = x.shape[0] // 2
            with_row[t] = jnp.concatenate([quadrants(x[:, : 2 * k]), quadrants(x[:, 2 * k :])], axis=1)
            t += 1


def prepare(at, first, second, groups):
    n_col = len(first)
    blk, k = first[0].shape
    n = n_col * blk
    tiles = sum(base.shape[0] for base, _ in groups)
    vmem = pl.BlockSpec(memory_space=VMEM)
    return pl.pallas_call(
        functools.partial(prepare_kernel, n_col),
        in_specs=[pl.BlockSpec(memory_space=pltpu.SMEM)] + [vmem] * (2 * n_col + 2 * len(groups)),
        out_specs=[vmem] * 3,
        out_shape=[
            jax.ShapeDtypeStruct((n, 2 * k), bf16),
            jax.ShapeDtypeStruct((tiles, k, 2 * k), f32),
            jax.ShapeDtypeStruct((k, k), f32),
        ],
        compiler_params=pltpu.CompilerParams(vmem_limit_bytes=36 * 1024 * 1024),
        cost_estimate=pl.CostEstimate(flops=12 * tiles * n * k * k, bytes_accessed=8 * tiles * n * k, transcendentals=0),
        name="prepare",
    )(at, *first, *second, *[x for pair in groups for x in pair])


def recompress_kernel(n, k, n_col, sizes, *refs):
    tiles = sum(sizes)
    place = [(g, j) for g, size in enumerate(sizes) for j in range(size)]
    groups = len(sizes)
    core_parts, refs = refs[:n_col], refs[n_col:]
    (small, with_row, row_row), refs = refs[:3], refs[3:]
    crosses, refs = refs[:groups], refs[groups:]
    bases, v_parts, refs = refs[:groups], refs[groups : 2 * groups], refs[2 * groups :]
    (w_parts, row_in, new_u, new_v), refs = refs[:4], refs[4:]
    s, tv, cu, sp, out, work, cross, cores, arrived, row_parts, sem, row_sem = refs
    root = math.sqrt(n)
    core_copies = [pltpu.make_async_copy(x, arrived.at[d], row_sem.at[1 + d]) for d, x in enumerate(core_parts)]
    row_copy = pltpu.make_async_copy(row_in, row_parts, row_sem.at[0])
    early, late, outs = [], [], []
    for t, (g, j) in enumerate(place):
        early.append(pltpu.make_async_copy(bases[g].at[j], s.at[t], sem.at[t]))
        late.append((
            pltpu.make_async_copy(v_parts[g].at[j], tv.at[t], sem.at[tiles + t]),
            pltpu.make_async_copy(w_parts.at[t], cu.at[t], sem.at[2 * tiles + t]),
        ))
        outs.append((
            pltpu.make_async_copy(s.at[t], new_u.at[t], sem.at[3 * tiles + t]),
            pltpu.make_async_copy(out.at[t], new_v.at[t], sem.at[4 * tiles + t]),
        ))
    for x in core_copies:
        x.start()
    row_copy.start()
    for x in early:
        x.start()
    for x in core_copies:
        x.wait()
    total = arrived[0]
    for d in range(1, n_col):
        total = total + arrived[d]
    cores[...] = total
    eye = jnp.where(
        lax.broadcasted_iota(jnp.int32, (k, k), 0) == lax.broadcasted_iota(jnp.int32, (k, k), 1), 1.0, 0.0
    ).astype(f32)
    mixes = [-product(cores[t], small[t]) for t in range(tiles)]
    row_copy.wait()
    for t, (g, j) in enumerate(place):
        early[t].wait()
        part = beside(s[t] + fold(mm(row_parts[...], doubled_rows(mixes[t]), NN)))
        sp[t] = part
        work[t, :, :k] = quadrants(mm(part, part, TN))
        work[t, :, k:] = eye
        x = product_tn(mixes[t], jnp.concatenate([with_row[t, :, k:], row_row[...]], axis=1))
        cross[t] = x + jnp.concatenate([crosses[g][j], with_row[t, :, :k].T], axis=1)
        for x in late[t]:
            x.start()
    eliminate(work, tiles, k)
    for t in range(tiles):
        inverse = work[t, :, k:]
        y = product(inverse, cross[t]) * (1.0 / root)
        c1 = y[:, :k]
        c2 = -product(y[:, k:], cores[t])
        by = doubled_columns(inverse * root)
        c12 = jnp.concatenate([doubled_columns(c1), doubled_columns(c2)], axis=1)
        for x in late[t]:
            x.wait()
        s[t] = fold(mm(sp[t], by, NT))
        outs[t][0].start()
        out[t] = fold(mm(jnp.concatenate([tv[t], cu[t]], axis=1), c12, NT))
        outs[t][1].start()
    for pair in outs:
        for x in pair:
            x.wait()


def recompress(core_parts, small, with_row, row_row, crosses, bases, v_parts, w_parts, row_parts):
    tiles, n, k2 = w_parts.shape
    k = k2 // 2
    n_col = len(core_parts)
    sizes = [x.shape[0] for x in bases]
    groups = len(sizes)
    any_ = pl.BlockSpec(memory_space=ANY)
    vmem = pl.BlockSpec(memory_space=VMEM)
    full = lambda: VMEM((tiles, n, k), f32)
    split = lambda: VMEM((tiles, n, 2 * k), bf16)
    return pl.pallas_call(
        functools.partial(recompress_kernel, n, k, n_col, sizes),
        in_specs=[any_] * n_col + [vmem] * (3 + groups) + [any_] * (2 * groups + 2),
        out_specs=[any_, any_],
        out_shape=[jax.ShapeDtypeStruct((tiles, n, k), f32)] * 2,
        scratch_shapes=[
            full(), split(), split(), split(), full(),
            VMEM((tiles, k, 2 * k), f32), VMEM((tiles, k, 2 * k), f32), VMEM((tiles, k, k), f32),
            VMEM((n_col, tiles, k, k), f32), VMEM((n, 2 * k), bf16),
            pltpu.SemaphoreType.DMA((5 * tiles,)), pltpu.SemaphoreType.DMA((1 + n_col,)),
        ],
        compiler_params=pltpu.CompilerParams(vmem_limit_bytes=44 * 1024 * 1024),
        cost_estimate=pl.CostEstimate(flops=24 * tiles * n * k * k, bytes_accessed=28 * tiles * n * k, transcendentals=0),
        name="recompress",
    )(*core_parts, small, with_row, row_row, *crosses, *bases, *v_parts, w_parts, row_parts)


def step(n_row, n_col, tile_u, tile_v, row_panel_u, row_panel_v, col_panel_u, col_panel_v, diag_inverse, sketch):
    chips = n_row // 2
    r, c = lax.axis_index("row"), lax.axis_index("col")
    at = jnp.stack([r, c]).astype(jnp.int32)
    chip = lax.shift_right_logical(r, 1)

    def partner(x, m):
        return lax.ppermute(x, "row", [(a, a ^ m) for a in range(n_row)])

    def shift(x, pairs):
        return lax.ppermute(x, "col", pairs)

    def around(x, d):
        return shift(x, [(a, (a + d) % n_col) for a in range(n_col)])

    def pick(x, i, axis=0):
        return lax.dynamic_index_in_dim(x, i, axis, keepdims=False)

    row_v, row_u = row_panel_v[0], row_panel_u[0]
    loads = [jnp.where(c + d < n_col, row_v, row_u) for d in range(1, n_col)]
    first = [around(x, d) for d, x in enumerate(loads, 1)]
    col_v_mine = jnp.stack([col_panel_v] + [partner(col_panel_v, 2 * e) for e in range(1, chips)])
    pair, rows, k = col_panel_u.shape
    cut = col_panel_u.reshape(pair, chips, rows // chips, k)
    cuts = jnp.stack([pick(cut, chip, 1)] + [partner(pick(cut, chip ^ e, 1), 2 * e) for e in range(1, chips)])
    col_v_other = partner(col_v_mine, 1)
    moved = [pick(cuts, chip ^ c)] + [around(pick(cuts, chip ^ lax.rem(c + d, n_col)), d) for d in range(1, n_col)]
    planes = lax.optimization_barrier(jnp.stack(moved))
    tiles = tile_u.shape[1]
    diag = split_diag(diag_inverse)
    groups = []
    for begin, end in ((0, 3 * tiles // 4), (3 * tiles // 4, tiles)):
        groups.append(sketch_tiles(tile_u[0], tile_v[0], sketch, begin, end))
    bases, v_parts, u_parts, crosses = zip(*groups)
    sums = solve(at, diag, row_u, [row_v] + first)
    second = [around(sums[d], n_col - d) for d in range(1, n_col)]
    gathered = [planes] + [partner(planes, 2 * e) for e in range(1, chips)]
    col_u_mine = jnp.stack(gathered)
    col_u_other = partner(col_u_mine, 1)
    w_parts, small = project(n_col, at, col_u_mine, col_u_other, sketch)
    cores = partial_cores(at, [sums[0]] + second, col_v_mine, col_v_other)
    core_parts = [cores[0]] + [around(cores[d], d) for d in range(1, n_col)]
    row_parts, with_row, row_row = prepare(at, [row_u] + first, [row_u] + second, list(zip(bases, u_parts)))
    new_u, new_v = recompress(core_parts, small, with_row, row_row, crosses, bases, v_parts, w_parts, row_parts)
    return new_u[None], new_v[None]


def solution(mesh):
    n_row, n_col = mesh.shape["row"], mesh.shape["col"]
    in_specs = (
        P("row", "col", None, None),
        P("row", "col", None, None),
        P("row", "col", None),
        P("row", "col", None),
        P("row", "col", None),
        P("row", "col", None),
        P("col", None),
        P(),
    )
    out_specs = (P("row", "col", None, None), P("row", "col", None, None))

    def body(*args):
        return step(n_row, n_col, *args)

    return jax.shard_map(body, mesh=mesh, in_specs=in_specs, out_specs=out_specs, check_vma=False)
```
